32 devices in a mesh: dp: 2 (over x), tp: 4 (over z), role: 4 (over y, core).
Axes of the slice: x: 2, y: 2, z: 4, core: 2. Of those that a mesh axis runs over, the one named last changes fastest.
Arguments:
- hidden: bfloat16 [2, 256, 2048], P(None, 'dp'), parts along dimension 1
- segment_ids: int32 [256], P('dp'), parts along dimension 0
- loss_mask: int32 [256], P('dp'), parts along dimension 0
- target: int32 [256], P('dp'), parts along dimension 0
- norm_gains: float32 [2, 3, 2048], replicated
- w_query: bfloat16 [4096, 2048], P(('role', 'tp'))
- b_query: bfloat16 [64, 64], P(('role', 'tp'))
- w_key: bfloat16 [1024, 2048], P('role')
- b_key: bfloat16 [16, 64], P('role')
- w_value: bfloat16 [1024, 2048], P('role')
- b_value: bfloat16 [16, 64], P('role')
- w_out: bfloat16 [4096, 2048], P(('role', 'tp'))
- w_gate: bfloat16 [16384, 2048], P(('role', 'tp'))
- w_up: bfloat16 [16384, 2048], P(('role', 'tp'))
- w_down: bfloat16 [16384, 2048], P(('role', 'tp'))
- w_head: bfloat16 [256512, 2048], P(('role', 'tp'))
Outputs:
- output 1: float32 [256], P('dp'), parts along dimension 0
- output 2: float32 [256], P('dp'), parts along dimension 0
There are 2 independent parts. The reference program is written for one: setup_inputs(seed, part) draws one part's arguments, and reference() takes and returns one part's arrays. A program takes and returns all parts, laid end to end along the dimension named above; an argument that names none is the same for every part.
All inputs are finite; a program needn't handle non-finite values.
Results may differ from the reference program's by a relative error of at most 0.00339183.
Values sent between devices are 32-bit elements.
A program may use at most 1 GiB of HBM per device.

```python
import jax
import jax.numpy as jnp
from jax import lax

TOKENS = 128
D = 2048
HEADS = 32
KV_HEADS = 8
HEAD = 64
FF = 8192
VOCAB = 128256
ROW_BLOCK = 32

EPS = 1e-6
ROPE_BASE = 1000000.0
TEMPERATURE = 0.7


def draw_pair(rng_key, shape, scale):
    base_key, diff_key = jax.random.split(rng_key)
    base_vals = jax.random.normal(base_key, shape, jnp.float32)
    diff_vals = jax.random.normal(diff_key, shape, jnp.float32)
    return jnp.concatenate([base_vals, 0.98 * base_vals + 0.2 * diff_vals], axis=0) * scale


def draw_segments(rng_key):
    mean_len = max(TOKENS // 4, 8)
    tok_index = jnp.arange(TOKENS)
    is_start = jax.random.randint(rng_key, (TOKENS,), 0, mean_len) == 0
    is_start = jnp.where(tok_index == 0, False, is_start)
    is_start = jnp.where(tok_index == TOKENS // 2, True, is_start)
    return jnp.cumsum(is_start.astype(jnp.int32)).astype(jnp.int32)


def setup_inputs(seed: int = 0, part: int = 0) -> dict:
    weight_keys = jax.random.split(jax.random.key(seed), 12)
    hid_keys = jax.random.split(jax.random.fold_in(jax.random.key(seed + 1), part), 2)
    int_keys = jax.random.split(jax.random.fold_in(jax.random.key(seed + 2), part), 3)
    base_hid = jax.random.normal(hid_keys[0], (TOKENS, D), jnp.float32)
    diff_hid = jax.random.normal(hid_keys[1], (TOKENS, D), jnp.float32)
    gain_base = jnp.array([1.0, 1.0, 2.0], jnp.float32).reshape(1, 3, 1)
    q_rows = HEADS * HEAD
    kv_rows = KV_HEADS * HEAD
    return {
        "hidden": jnp.stack([base_hid, 0.95 * base_hid + 0.3 * diff_hid]).astype(jnp.bfloat16),
        "segment_ids": draw_segments(int_keys[0]),
        "loss_mask": (jax.random.randint(int_keys[1], (TOKENS,), 0, 8) > 0).astype(jnp.int32),
        "target": jax.random.randint(int_keys[2], (TOKENS,), 0, VOCAB).astype(jnp.int32),
        "norm_gains": draw_pair(weight_keys[0], (1, 3, D), 0.2) + gain_base,
        "w_query": draw_pair(weight_keys[1], (q_rows, D), D ** -0.5).astype(jnp.bfloat16),
        "b_query": draw_pair(weight_keys[2], (HEADS, HEAD), 0.5).astype(jnp.bfloat16),
        "w_key": draw_pair(weight_keys[3], (kv_rows, D), D ** -0.5).astype(jnp.bfloat16),
        "b_key": draw_pair(weight_keys[4], (KV_HEADS, HEAD), 0.5).astype(jnp.bfloat16),
        "w_value": draw_pair(weight_keys[5], (kv_rows, D), D ** -0.5).astype(jnp.bfloat16),
        "b_value": draw_pair(weight_keys[6], (KV_HEADS, HEAD), 0.5).astype(jnp.bfloat16),
        "w_out": draw_pair(weight_keys[7], (q_rows, D), 2.5 * q_rows ** -0.5).astype(jnp.bfloat16),
        "w_gate": draw_pair(weight_keys[8], (FF, D), D ** -0.5).astype(jnp.bfloat16),
        "w_up": draw_pair(weight_keys[9], (FF, D), D ** -0.5).astype(jnp.bfloat16),
        "w_down": draw_pair(weight_keys[10], (FF, D), 1.5 * FF ** -0.5).astype(jnp.bfloat16),
        "w_head": draw_pair(weight_keys[11], (VOCAB, D), D ** -0.5).astype(jnp.bfloat16),
    }


def rms_norm(values, gain):
    vals_f32 = values.astype(jnp.float32)
    inv_rms = lax.rsqrt(jnp.mean(vals_f32 * vals_f32, axis=-1, keepdims=True) + EPS)
    return (vals_f32 * inv_rms * gain).astype(jnp.bfloat16)


def segment_positions(segment_ids):
    tok_index = jnp.arange(segment_ids.shape[-1])
    prev_ids = jnp.concatenate([segment_ids[..., :1] - 1, segment_ids[..., :-1]], axis=-1)
    seg_start = lax.cummax(jnp.where(segment_ids != prev_ids, tok_index, 0), axis=segment_ids.ndim - 1)
    return tok_index - seg_start


def rotary(values, positions):
    half_dim = values.shape[-1] // 2
    inv_freq = ROPE_BASE ** (-2.0 * jnp.arange(half_dim).astype(jnp.float32) / values.shape[-1])
    angles = positions.astype(jnp.float32)[..., None] * inv_freq
    cos_part = jnp.cos(angles)[..., None, :]
    sin_part = jnp.sin(angles)[..., None, :]
    first_half = values[..., :half_dim]
    second_half = values[..., half_dim:]
    return jnp.concatenate([first_half * cos_part - second_half * sin_part, second_half * cos_part + first_half * sin_part], axis=-1)


def model_layer(x_in, segment_ids, gain3, w_query, b_query, w_key, b_key, w_value, b_value, w_out, w_gate, w_up, w_down):
    positions = segment_positions(segment_ids)
    tok_index = jnp.arange(TOKENS)
    allowed = (segment_ids[:, None] == segment_ids[None, :]) & (tok_index[:, None] >= tok_index[None, :])
    normed = rms_norm(x_in, gain3[0])
    q_proj = jnp.dot(normed, w_query.T, preferred_element_type=jnp.float32).reshape(TOKENS, HEADS, HEAD) + b_query.astype(jnp.float32)
    k_proj = jnp.dot(normed, w_key.T, preferred_element_type=jnp.float32).reshape(TOKENS, KV_HEADS, HEAD) + b_key.astype(jnp.float32)
    v_proj = (jnp.dot(normed, w_value.T, preferred_element_type=jnp.float32).reshape(TOKENS, KV_HEADS, HEAD) + b_value.astype(jnp.float32)).astype(jnp.bfloat16)
    q_rot = rotary(q_proj, positions).astype(jnp.bfloat16)
    k_rot = rotary(k_proj, positions).astype(jnp.bfloat16)
    q_grouped = jnp.moveaxis(q_rot.reshape(TOKENS, KV_HEADS, HEADS // KV_HEADS, HEAD), 1, 0)

    def one_group(group_args):
        q_group, k_group, v_group = group_args
        scores = jnp.einsum("tgd,sd->gts", q_group.astype(jnp.float32), k_group.astype(jnp.float32)) * HEAD ** -0.5
        scores = jnp.where(allowed[None], scores, -1e30)
        attn_probs = jax.nn.softmax(scores, axis=-1).astype(jnp.bfloat16)
        return jnp.einsum("gts,sd->tgd", attn_probs.astype(jnp.float32), v_group.astype(jnp.float32)).astype(jnp.bfloat16)

    attn = lax.map(one_group, (q_grouped, jnp.moveaxis(k_rot, 1, 0), jnp.moveaxis(v_proj, 1, 0)))
    attn = jnp.moveaxis(attn, 0, 1).reshape(TOKENS, HEADS * HEAD)
    resid = (x_in.astype(jnp.float32) + jnp.dot(attn, w_out, preferred_element_type=jnp.float32)).astype(jnp.bfloat16)
    normed_mlp = rms_norm(resid, gain3[1])
    gate_proj = jnp.dot(normed_mlp, w_gate.T, preferred_element_type=jnp.float32)
    up_proj = jnp.dot(normed_mlp, w_up.T, preferred_element_type=jnp.float32)
    act_vals = (jax.nn.silu(gate_proj) * up_proj).astype(jnp.bfloat16)
    layer_out = (resid.astype(jnp.float32) + jnp.dot(act_vals, w_down, preferred_element_type=jnp.float32)).astype(jnp.bfloat16)
    return rms_norm(layer_out, gain3[2])


def reference(hidden, segment_ids, loss_mask, target, norm_gains, w_query, b_query, w_key, b_key, w_value, b_value, w_out, w_gate, w_up, w_down, w_head):
    q_rows = HEADS * HEAD
    kv_rows = KV_HEADS * HEAD
    finals = []
    for model_idx in range(2):
        q_lo = model_idx * q_rows
        kv_lo = model_idx * kv_rows
        ff_lo = model_idx * FF
        finals.append(model_layer(
            hidden[model_idx], segment_ids, norm_gains[model_idx],
            w_query[q_lo:q_lo + q_rows], b_query[model_idx * HEADS:(model_idx + 1) * HEADS],
            w_key[kv_lo:kv_lo + kv_rows], b_key[model_idx * KV_HEADS:(model_idx + 1) * KV_HEADS],
            w_value[kv_lo:kv_lo + kv_rows], b_value[model_idx * KV_HEADS:(model_idx + 1) * KV_HEADS],
            w_out[q_lo:q_lo + q_rows], w_gate[ff_lo:ff_lo + FF], w_up[ff_lo:ff_lo + FF], w_down[ff_lo:ff_lo + FF]))
    head_pol = w_head[:VOCAB]
    head_ref = w_head[VOCAB:]
    num_blocks = TOKENS // ROW_BLOCK
    vocab_ids = jnp.arange(VOCAB)

    def head_block(block_args):
        pol_rows, ref_rows, tgt_rows = block_args
        pol_lp = jax.nn.log_softmax(jnp.dot(pol_rows, head_pol.T, preferred_element_type=jnp.float32) / TEMPERATURE, axis=-1)
        ref_lp = jax.nn.log_softmax(jnp.dot(ref_rows, head_ref.T, preferred_element_type=jnp.float32) / TEMPERATURE, axis=-1)
        kl_rows = jnp.sum(jnp.exp(pol_lp) * (pol_lp - ref_lp), axis=-1)
        tgt_lp = jnp.sum(jnp.where(vocab_ids[None, :] == tgt_rows[:, None], pol_lp, 0.0), axis=-1)
        return kl_rows, tgt_lp

    kl_div, target_logp = lax.map(head_block, (finals[0].reshape(num_blocks, ROW_BLOCK, D), finals[1].reshape(num_blocks, ROW_BLOCK, D), target.reshape(num_blocks, ROW_BLOCK)))
    mask_vals = loss_mask.astype(jnp.float32)
    return kl_div.reshape(TOKENS) * mask_vals, target_logp.reshape(TOKENS) * mask_vals
```

```python
import functools
import math

import jax
import jax.numpy as jnp
from jax import lax
from jax.experimental import pallas as pl
from jax.experimental.pallas import tpu as pltpu
from jax.sharding import PartitionSpec as P

MESH = pl.DeviceIdType.MESH
F32 = jnp.float32
BF16 = jnp.bfloat16
EPS = 1e-6
LOG_BASE = math.log(1000000.0)
INV_TEMP = 1.0 / 0.7

TOK = 128
D = 2048
DH = D // 2
HEAD = 64
QH = 4
FF = 1024
VOC = 16032
MID = VOC // 2
C = 576
NCH = 14
BLK = C * NCH
OFF = VOC - BLK
LAP = BLK - MID
NBUF = 4
NB = 1
N = TOK // NB
PK = TOK // N
CP = C // PK
NZ = 4
NQ = N // NZ
NEG = -1e30


def dot(lhs, rhs):
    return jnp.dot(lhs, rhs, preferred_element_type=F32)


def kernel(hid, wq, wk, wv, wo, wg, wu, wd, wh, gains, seg, mask, target, bq, bk, bv,
           kl_out, lp_out,
           xb, wqkv, wob, wgb, wub, wdb, wbuf, tr, act_t, part, core_in, chip_sum, rs_in, gath, resid, hid_t, hid_all,
           u_buf, zsend, zrecv, zkeep, stat, stats_in,
           in_sem, w_sem, d_s, d_r, rs_s, rs_r, ag_s, ag_r, rl_s, rl_r, y_s, y_r, f_s, f_r):
    dp, tp, ro = lax.axis_index("dp"), lax.axis_index("tp"), lax.axis_index("role")
    half, core = ro // 2, ro % 2
    shard = core * NZ + tp
    me = tp * 4 + ro
    pol = half == 0
    partner = (dp, tp, ro + 1 - 2 * core)
    across = (dp, tp, (ro + 2) % 4)

    def z_peer(k):
        return (dp, (tp + k) % NZ, ro)

    def rel_peer(k):
        other = (me + k) % 16
        return (dp, other // 4, other % 4)

    loads = [
        pltpu.make_async_copy(hid.at[half], xb, in_sem.at[0]),
        pltpu.make_async_copy(wq, wqkv.at[pl.ds(0, 256)], in_sem.at[1]),
        pltpu.make_async_copy(wk.at[pl.ds(pl.multiple_of(tp * HEAD, HEAD), HEAD)], wqkv.at[pl.ds(256, HEAD)], in_sem.at[2]),
        pltpu.make_async_copy(wv.at[pl.ds(pl.multiple_of(tp * HEAD, HEAD), HEAD)], wqkv.at[pl.ds(320, HEAD)], in_sem.at[3]),
        pltpu.make_async_copy(wo, wob, in_sem.at[4]),
        pltpu.make_async_copy(wg, wgb, in_sem.at[5]),
        pltpu.make_async_copy(wu, wub, in_sem.at[6]),
        pltpu.make_async_copy(wd, wdb, in_sem.at[7]),
    ]
    for copy in loads:
        copy.start()

    barrier = pltpu.get_barrier_semaphore()
    for k in range(1, 16):
        pl.semaphore_signal(barrier, inc=1, device_id=rel_peer(k), device_id_type=MESH)

    send_base = half * OFF
    keep_base = (1 - half) * OFF

    def w_load(g):
        kept = g // NCH >= NB
        base = jnp.where(kept, keep_base, send_base) + (g % NCH) * C
        slot = g % NBUF
        return pltpu.make_async_copy(wh.at[pl.ds(pl.multiple_of(base, 16), C)], wbuf.at[slot], w_sem.at[slot])

    for g in range(NBUF):
        w_load(g).start()

    rows8 = lax.broadcasted_iota(jnp.int32, (QH, HEAD), 0)
    tr[...] = jnp.zeros_like(tr)
    tr[0:QH, 0:HEAD] = bq[...].astype(F32)
    pick = rows8 == tp
    tr[QH:QH + 1, 0:HEAD] = jnp.sum(jnp.where(pick, bk[...].astype(F32), 0.0), axis=0, keepdims=True)
    tr[QH + 1:QH + 2, 0:HEAD] = jnp.sum(jnp.where(pick, bv[...].astype(F32), 0.0), axis=0, keepdims=True)
    seg_row = seg[...].astype(F32)
    tr[QH + 2:QH + 3, :] = seg_row
    cols = jnp.transpose(tr[...])
    seg_col = cols[:, QH + 2:QH + 3]
    src_id = lax.broadcasted_iota(jnp.int32, (TOK, TOK), 0)
    dst_id = lax.broadcasted_iota(jnp.int32, (TOK, TOK), 1)
    allowed = (seg_col == seg_row) & (src_id <= dst_id)
    pos = jnp.sum(jnp.where(allowed, 1.0, 0.0), axis=0, keepdims=True) - 1.0
    rot_id = lax.broadcasted_iota(jnp.int32, (HEAD // 2, TOK), 0).astype(F32)
    angles = pos * jnp.exp(rot_id * (-2.0 * LOG_BASE / HEAD))
    cos_part, sin_part = jnp.cos(angles), jnp.sin(angles)

    def normed(rows, gain):
        inv = lax.rsqrt(jnp.mean(rows * rows, axis=-1, keepdims=True) + EPS)
        return rows * inv * gain

    gain = gains[half]
    loads[0].wait()
    act_t[...] = jnp.transpose(normed(xb[...].astype(F32), gain[0:1])).astype(BF16)
    for copy in loads[1:4]:
        copy.wait()
    qkv = dot(wqkv[...], act_t[...])

    def rotate(vals):
        lo, hi = vals[:HEAD // 2], vals[HEAD // 2:]
        return jnp.concatenate([lo * cos_part - hi * sin_part, hi * cos_part + lo * sin_part], axis=0)

    queries = []
    for h in range(QH):
        q_h = qkv[h * HEAD:(h + 1) * HEAD] + cols[0:HEAD, h:h + 1]
        queries.append(rotate(q_h).astype(BF16))
    q_cat = jnp.concatenate(queries, axis=1)
    key = jnp.transpose(rotate(qkv[256:320] + cols[0:HEAD, QH:QH + 1])).astype(BF16)
    val_t = (qkv[320:384] + cols[0:HEAD, QH + 1:QH + 2]).astype(BF16)
    scores = dot(key, q_cat) * (HEAD ** -0.5)
    scores = jnp.where(jnp.concatenate([allowed] * QH, axis=1), scores, NEG)
    weights = jnp.exp(scores - jnp.max(scores, axis=0, keepdims=True))
    probs = (weights / jnp.sum(weights, axis=0, keepdims=True)).astype(BF16)
    out_t = dot(val_t, probs)
    attn = jnp.transpose(jnp.concatenate([out_t[:, h * TOK:(h + 1) * TOK] for h in range(QH)], axis=0)).astype(BF16)
    loads[4].wait()
    pl.semaphore_wait(barrier, 15)

    def copies_core(i):
        return pltpu.make_async_remote_copy(
            src_ref=part.at[i, 1 - core], dst_ref=core_in.at[i], send_sem=d_s.at[i], recv_sem=d_r.at[i],
            device_id=partner, device_id_type=MESH)

    def copies_rs(i, k):
        return pltpu.make_async_remote_copy(
            src_ref=chip_sum.at[i, (tp + k) % NZ], dst_ref=rs_in.at[i, k - 1],
            send_sem=rs_s.at[i, k - 1], recv_sem=rs_r.at[i, k - 1], device_id=z_peer(k), device_id_type=MESH)

    def copies_ag(i, k, owner):
        return pltpu.make_async_remote_copy(
            src_ref=gath.at[i, core, owner], dst_ref=gath.at[i, core, owner],
            send_sem=ag_s.at[i, k - 1], recv_sem=ag_r.at[i, k - 1], device_id=z_peer(k), device_id_type=MESH)

    def copies_relay(i, k, side):
        owner = (tp + NZ - k) % NZ
        return pltpu.make_async_remote_copy(
            src_ref=gath.at[i, side, owner], dst_ref=gath.at[i, side, owner],
            send_sem=rl_s.at[i, k], recv_sem=rl_r.at[i, k], device_id=partner, device_id_type=MESH)

    def ar_start(i, partial):
        part[i, 0] = partial[:, :DH]
        part[i, 1] = partial[:, DH:]
        copies_core(i).start()

    def ar_chip(i):
        copies_core(i).wait_recv()
        chip_sum[i] = (part[i, core] + core_in[i]).reshape(NZ, NQ, DH)
        for k in (2, 1, 3):
            copies_rs(i, k).start()

    def ar_own(i, before):
        for k in (1, 2, 3):
            copies_rs(i, k).wait_recv()
        total = chip_sum[i, tp] + rs_in[i, 0] + rs_in[i, 1] + rs_in[i, 2]
        gath[i, core, tp] = (before + total).astype(BF16).astype(F32)
        for k in (2, 1, 3):
            copies_ag(i, k, tp).start()
        copies_relay(i, 0, core).start()

    def ar_relay(i):
        for k in (1, 2, 3):
            copies_ag(i, k, (tp + NZ - k) % NZ).wait_recv()
            copies_relay(i, k, core).start()

    def ar_rows(i):
        for k in range(4):
            copies_relay(i, k, 1 - core).wait_recv()
        return jnp.concatenate([gath[i, 0].reshape(N, DH), gath[i, 1].reshape(N, DH)], axis=1)

    def ar_drain(i):
        copies_core(i).wait_send()
        for k in (1, 2, 3):
            copies_rs(i, k).wait_send()
            copies_ag(i, k, tp).wait_send()
        for k in range(4):
            copies_relay(i, k, core).wait_send()

    first = dot(attn, wob[...])
    for b in range(NB):
        ar_start(b, first[b * N:(b + 1) * N])

    def own_x(b):
        row0 = pl.multiple_of(b * N + tp * NQ, 8)
        return jnp.where(core == 0, xb[pl.ds(row0, NQ), 0:DH].astype(F32), xb[pl.ds(row0, NQ), DH:D].astype(F32))

    def mlp(b):
        rows = ar_rows(b)
        b_t = jnp.transpose(jnp.concatenate([normed(rows, gain[1:2])] * PK, axis=0)).astype(BF16)
        act_t[...] = b_t
        if b == 0:
            for copy in loads[5:8]:
                copy.wait()
        for j in range(4):
            gate = dot(wgb[j * 256:(j + 1) * 256], act_t[...])
            up = dot(wub[j * 256:(j + 1) * 256], act_t[...])
            u_t = gate * (1.0 / (1.0 + jnp.exp(-gate))) * up
            u_buf[:, j * 256:(j + 1) * 256] = jnp.transpose(u_t).astype(BF16)
        ar_start(NB + b, dot(u_buf[0:N], wdb[...]))

    def own_resid(b):
        return gath[b, core, tp]

    def final_rows(b):
        rows = ar_rows(NB + b)
        return normed(rows, gain[2:3])

    lane = lax.broadcasted_iota(jnp.int32, (1, TOK), 1)
    tgt_row = target[...] - shard * VOC

    M_OWN, S_OWN, M_C, S_C, TGT = 0, 1, 2, 3, 4
    stat[...] = jnp.where(lax.broadcasted_iota(jnp.int32, stat.shape, 0) % 2 == 0, NEG, 0.0)
    stat[TGT:TGT + 1] = jnp.zeros((1, TOK), F32)

    def own_update(z, rows, base_row, lo, hi):
        live = (rows >= lo) & (rows < hi)
        zm = jnp.where(live, z, NEG)
        m_old = stat[M_OWN:M_OWN + 1]
        m_new = jnp.maximum(m_old, jnp.max(zm, axis=0, keepdims=True))
        s_add = jnp.sum(jnp.exp(zm - m_new), axis=0, keepdims=True)
        stat[S_OWN:S_OWN + 1] = stat[S_OWN:S_OWN + 1] * jnp.exp(m_old - m_new) + s_add
        stat[M_OWN:M_OWN + 1] = m_new
        hit = live & (rows == tgt_row - base_row)
        stat[TGT:TGT + 1] = stat[TGT:TGT + 1] + jnp.sum(jnp.where(hit, z, 0.0), axis=0, keepdims=True)

    row_id = lax.broadcasted_iota(jnp.int32, (C, TOK), 0)

    def y_copy(g):
        b, i = g // NCH, g % NCH
        return pltpu.make_async_remote_copy(
            src_ref=zsend.at[b, i], dst_ref=zrecv.at[b, i], send_sem=y_s.at[g], recv_sem=y_r.at[g],
            device_id=across, device_id_type=MESH)

    def next_load(g):
        @pl.when(g + NBUF < (NB + 1) * NCH)
        def _():
            w_load(g + NBUF).start()

    def send_chunk(i, carry):
        g = i
        w_load(g).wait()
        z = dot(wbuf[g % NBUF], hid_t[...]) * INV_TEMP
        zsend[0, i] = z
        y_copy(g).start()
        next_load(g)
        own_update(z, row_id + i * C, send_base, half * LAP, MID + half * LAP)
        return carry

    keep_lo = (1 - half) * LAP
    keep_hi = MID + (1 - half) * LAP

    def keep_chunk(i, carry):
        g = NB * NCH + i
        w_load(g).wait()
        z = dot(wbuf[g % NBUF], hid_t[...]) * INV_TEMP
        zkeep[i] = z
        next_load(g)
        own_update(z, row_id + i * C, keep_base, keep_lo, keep_hi)
        return carry

    def pair_chunk(i, carry):
        y_copy(i).wait_recv()
        rows = row_id + i * C
        live = (rows >= keep_lo) & (rows < keep_hi)
        own, other = zkeep[i], zrecv[0, i]
        z0 = jnp.where(pol, own, other)
        diff = jnp.where(pol, own - other, other - own)
        zm = jnp.where(live, z0, NEG)
        m_old = stat[M_C:M_C + 1]
        m_new = jnp.maximum(m_old, jnp.max(zm, axis=0, keepdims=True))
        add = jnp.sum(jnp.exp(zm - m_new) * diff, axis=0, keepdims=True)
        stat[S_C:S_C + 1] = stat[S_C:S_C + 1] * jnp.exp(m_old - m_new) + add
        stat[M_C:M_C + 1] = m_new
        return carry

    ar_chip(0)
    ar_own(0, own_x(0))
    ar_relay(0)
    mlp(0)
    ar_chip(1)
    ar_own(1, own_resid(0))
    ar_relay(1)
    hid_t[...] = jnp.transpose(final_rows(0)).astype(BF16)
    lax.fori_loop(0, NCH, send_chunk, 0)
    lax.fori_loop(0, NCH, keep_chunk, 0)
    lax.fori_loop(0, NCH, pair_chunk, 0)

    def stat_copy(k, slot):
        return pltpu.make_async_remote_copy(
            src_ref=stat, dst_ref=stats_in.at[slot], send_sem=f_s.at[k - 1], recv_sem=f_r.at[k - 1],
            device_id=rel_peer(k), device_id_type=MESH)

    for k in range(1, 16):
        stat_copy(k, me).start()
    stats_in[me] = stat[...]
    for k in range(1, 16):
        stat_copy(k, (me + 16 - k) % 16).wait_recv()

    def lse(model):
        ids = [i for i in range(16) if (i % 4) // 2 == model]
        top = functools.reduce(jnp.maximum, [stats_in[i, M_OWN:M_OWN + 1] for i in ids])
        tot = sum(stats_in[i, S_OWN:S_OWN + 1] * jnp.exp(stats_in[i, M_OWN:M_OWN + 1] - top) for i in ids)
        return top, tot

    top0, tot0 = lse(0)
    top1, tot1 = lse(1)
    lse0, lse1 = top0 + jnp.log(tot0), top1 + jnp.log(tot1)
    cross = sum(stats_in[i, S_C:S_C + 1] * jnp.exp(stats_in[i, M_C:M_C + 1] - top0) for i in range(16))
    tgt_z = sum(stats_in[i, TGT:TGT + 1] for i in range(16) if (i % 4) // 2 == 0)
    found = mask[...].astype(F32)
    kl_out[...] = found * (cross / tot0 - lse0 + lse1)
    lp_out[...] = found * (tgt_z - lse0)

    for i in range(2 * NB):
        ar_drain(i)

    def drain(g, carry):
        y_copy(g).wait_send()
        return carry

    lax.fori_loop(0, NB * NCH, drain, 0)
    for k in range(1, 16):
        stat_copy(k, me).wait_send()


def solution(mesh):
    by_shard = P(("role", "tp"), None)
    by_role = P("role", None)

    def per_device(hidden, segment_ids, loss_mask, target, norm_gains, w_query, b_query, w_key, b_key, w_value, b_value, w_out, w_gate, w_up, w_down, w_head):
        anywhere = pl.BlockSpec(memory_space=pl.ANY)
        vmem = pl.BlockSpec(memory_space=pltpu.VMEM)
        dma = pltpu.SemaphoreType.DMA
        kl, lp = pl.pallas_call(
            kernel,
            out_shape=(jax.ShapeDtypeStruct((1, TOK), F32),) * 2,
            in_specs=[anywhere] * 9 + [vmem] * 7,
            out_specs=(vmem, vmem),
            scratch_shapes=[
                pltpu.VMEM((TOK, D), BF16),
                pltpu.VMEM((384, D), BF16),
                pltpu.VMEM((256, D), BF16),
                pltpu.VMEM((FF, D), BF16),
                pltpu.VMEM((FF, D), BF16),
                pltpu.VMEM((FF, D), BF16),
                pltpu.VMEM((NBUF, C, D), BF16),
                pltpu.VMEM((TOK, TOK), F32),
                pltpu.VMEM((D, TOK), BF16),
                pltpu.VMEM((2 * NB, 2, N, DH), F32),
                pltpu.VMEM((2 * NB, N, DH), F32),
                pltpu.VMEM((2 * NB, NZ, NQ, DH), F32),
                pltpu.VMEM((2 * NB, NZ - 1, NQ, DH), F32),
                pltpu.VMEM((2 * NB, 2, NZ, NQ, DH), F32),
                pltpu.VMEM((8, TOK), F32),
                pltpu.VMEM((D, TOK), BF16),
                pltpu.VMEM((8, TOK), F32),
                pltpu.VMEM((TOK, FF), BF16),
                pltpu.VMEM((NB, NCH, CP, TOK), F32),
                pltpu.VMEM((NB, NCH, CP, TOK), F32),
                pltpu.VMEM((NCH, C, TOK), F32),
                pltpu.VMEM((8, TOK), F32),
                pltpu.VMEM((16, 8, TOK), F32),
                dma((8,)), dma((NBUF,)),
                dma((2 * NB,)), dma((2 * NB,)),
                dma((2 * NB, 3)), dma((2 * NB, 3)),
                dma((2 * NB, 3)), dma((2 * NB, 3)),
                dma((2 * NB, 4)), dma((2 * NB, 4)),
                dma((NB * NCH,)), dma((NB * NCH,)),
                dma((15,)), dma((15,)),
            ],
            compiler_params=pltpu.CompilerParams(
                collective_id=0, has_side_effects=True, vmem_limit_bytes=60 * 1024 * 1024),
        )(hidden, w_query, w_key, w_value, w_out, w_gate, w_up, w_down, w_head, norm_gains,
          segment_ids.reshape(1, TOK), loss_mask.reshape(1, TOK), target.reshape(1, TOK), b_query, b_key, b_value)
        return kl.reshape(TOK), lp.reshape(TOK)

    in_specs = (P(None, "dp", None), P("dp"), P("dp"), P("dp"), P(None, None, None), by_shard, by_shard, by_role, by_role, by_role, by_role, by_shard, by_shard, by_shard, by_shard, by_shard)
    return jax.shard_map(per_device, mesh=mesh, in_specs=in_specs, out_specs=(P("dp"), P("dp")), check_vma=False)
```

```python
import functools
import math

import jax
import jax.numpy as jnp
from jax import lax
from jax.experimental import pallas as pl
from jax.experimental.pallas import tpu as pltpu
from jax.sharding import PartitionSpec as P

MESH = pl.DeviceIdType.MESH
F32 = jnp.float32
BF16 = jnp.bfloat16
EPS = 1e-6
LOG_BASE = math.log(1000000.0)
INV_TEMP = 1.0 / 0.7

TOK = 128
D = 2048
DH = D // 2
HEAD = 64
QH = 4
FF = 1024
VOC = 16032
MID = VOC // 2
C = 576
NCH = 14
BLK = C * NCH
OFF = VOC - BLK
LAP = BLK - MID
NBUF = 4
NB = 4
N = TOK // NB
PK = TOK // N
CP = C // PK
NZ = 4
NQ = N // NZ
NEG = -1e30
ORDER = (
    (0, 0), (1, 0), (0, 1), (1, 1), (2, 0), (0, 2), (0, 3), (1, 2), (0, 4), (1, 3), (1, 4), (0, 5), (2, 1), (0, 6), (0, 7),
    (0, 0, 5), (1, 5), (3, 0), (0, 5, 10), (1, 6), (2, 2), (2, 3), (0, 10, 14), (1, 7), (2, 4), (3, 1),
    (1, 0, 5), (2, 5), (3, 2), (3, 3), (1, 5, 10), (2, 6), (3, 4), (2, 7), (1, 10, 14), (3, 5),
    (2, 0, 7), (3, 6), (3, 7), (2, 7, 14), (3, 0, 14),
)


def dot(lhs, rhs):
    return jnp.dot(lhs, rhs, preferred_element_type=F32)


def kernel(hid, wq, wk, wv, wo, wg, wu, wd, wh, gains, seg, target, bq, bk, bv,
           out,
           xb, gain_in, wqkv, wob, wgb, wub, wdb, wbuf, tr, act_t, part, core_in, chip_sum, rs_in, gath, hid_t, hid_all,
           u_buf, zsend, zrecv, zkeep, stat, stats_in,
           in_sem, w_sem, d_s, d_r, rs_s, rs_r, ag_s, ag_r, rl_s, rl_r, y_s, y_r, f_s, f_r):
    dp, tp, ro = lax.axis_index("dp"), lax.axis_index("tp"), lax.axis_index("role")
    half, core = ro // 2, ro % 2
    shard = core * NZ + tp
    me = tp * 4 + ro
    pol = half == 0
    partner = (dp, tp, ro + 1 - 2 * core)
    across = (dp, tp, (ro + 2) % 4)

    def z_peer(k):
        return (dp, (tp + k) % NZ, ro)

    def rel_peer(k):
        other = (me + k) % 16
        return (dp, other // 4, other % 4)

    loads = [
        pltpu.make_async_copy(hid.at[half], xb, in_sem.at[0]),
        pltpu.make_async_copy(wq, wqkv.at[pl.ds(0, 256)], in_sem.at[1]),
        pltpu.make_async_copy(wk.at[pl.ds(pl.multiple_of(tp * HEAD, HEAD), HEAD)], wqkv.at[pl.ds(256, HEAD)], in_sem.at[2]),
        pltpu.make_async_copy(wv.at[pl.ds(pl.multiple_of(tp * HEAD, HEAD), HEAD)], wqkv.at[pl.ds(320, HEAD)], in_sem.at[3]),
        pltpu.make_async_copy(wo, wob, in_sem.at[4]),
        pltpu.make_async_copy(wg, wgb, in_sem.at[5]),
        pltpu.make_async_copy(wu, wub, in_sem.at[6]),
        pltpu.make_async_copy(wd, wdb, in_sem.at[7]),
        pltpu.make_async_copy(gains, gain_in, in_sem.at[8]),
    ]
    first_loads = loads[0:4] + loads[8:9]
    for copy in first_loads:
        copy.start()

    barrier = pltpu.get_barrier_semaphore()
    for k in range(1, 16):
        pl.semaphore_signal(barrier, inc=1, device_id=rel_peer(k), device_id_type=MESH)

    send_base = half * OFF
    keep_base = (1 - half) * OFF

    def w_load(g):
        kept = g // NCH >= NB
        base = jnp.where(kept, keep_base, send_base) + (g % NCH) * C
        slot = g % NBUF
        return pltpu.make_async_copy(wh.at[pl.ds(pl.multiple_of(base, 16), C)], wbuf.at[slot], w_sem.at[slot])

    rows8 = lax.broadcasted_iota(jnp.int32, (QH, HEAD), 0)
    tr[...] = jnp.zeros_like(tr)
    tr[0:QH, 0:HEAD] = bq[...].astype(F32)
    pick = rows8 == tp
    tr[QH:QH + 1, 0:HEAD] = jnp.sum(jnp.where(pick, bk[...].astype(F32), 0.0), axis=0, keepdims=True)
    tr[QH + 1:QH + 2, 0:HEAD] = jnp.sum(jnp.where(pick, bv[...].astype(F32), 0.0), axis=0, keepdims=True)
    seg_row = seg[...].astype(F32)
    tr[QH + 2:QH + 3, :] = seg_row
    cols = jnp.transpose(tr[...])
    seg_col = cols[:, QH + 2:QH + 3]
    src_id = lax.broadcasted_iota(jnp.int32, (TOK, TOK), 0)
    dst_id = lax.broadcasted_iota(jnp.int32, (TOK, TOK), 1)
    allowed = (seg_col == seg_row) & (src_id <= dst_id)
    pos = jnp.sum(jnp.where(allowed, 1.0, 0.0), axis=0, keepdims=True) - 1.0
    rot_id = lax.broadcasted_iota(jnp.int32, (HEAD // 2, TOK), 0).astype(F32)
    angles = pos * jnp.exp(rot_id * (-2.0 * LOG_BASE / HEAD))
    cos_part, sin_part = jnp.cos(angles), jnp.sin(angles)

    def normed(rows, scale):
        inv = lax.rsqrt(jnp.mean(rows * rows, axis=-1, keepdims=True) + EPS)
        return rows * inv * scale

    loads[0].wait()
    loads[8].wait()

    def gain(k):
        return jnp.where(pol, gain_in[k, 0:1], gain_in[k, 1:2])

    act_t[...] = jnp.transpose(normed(xb[...].astype(F32), gain(0))).astype(BF16)
    for copy in loads[1:4]:
        copy.wait()
    for copy in loads[4:8]:
        copy.start()
    for g in range(NBUF):
        w_load(g).start()
    qkv = dot(wqkv[...], act_t[...])

    def rotate(vals):
        lo, hi = vals[:HEAD // 2], vals[HEAD // 2:]
        return jnp.concatenate([lo * cos_part - hi * sin_part, hi * cos_part + lo * sin_part], axis=0)

    queries = []
    for h in range(QH):
        q_h = qkv[h * HEAD:(h + 1) * HEAD] + cols[0:HEAD, h:h + 1]
        queries.append(rotate(q_h).astype(BF16))
    q_cat = jnp.concatenate(queries, axis=1)
    key = jnp.transpose(rotate(qkv[256:320] + cols[0:HEAD, QH:QH + 1])).astype(BF16)
    val_t = (qkv[320:384] + cols[0:HEAD, QH + 1:QH + 2]).astype(BF16)
    scores = dot(key, q_cat) * (HEAD ** -0.5)
    scores = jnp.where(jnp.concatenate([allowed] * QH, axis=1), scores, NEG)
    weights = jnp.exp(scores - jnp.max(scores, axis=0, keepdims=True))
    probs = (weights / jnp.sum(weights, axis=0, keepdims=True)).astype(BF16)
    out_t = dot(val_t, probs)
    attn = jnp.transpose(jnp.concatenate([out_t[:, h * TOK:(h + 1) * TOK] for h in range(QH)], axis=0)).astype(BF16)
    loads[4].wait()
    pl.semaphore_wait(barrier, 15)

    def copies_core(i):
        return pltpu.make_async_remote_copy(
            src_ref=part.at[i, 1 - core], dst_ref=core_in.at[i], send_sem=d_s.at[i], recv_sem=d_r.at[i],
            device_id=partner, device_id_type=MESH)

    def copies_rs(i, k):
        return pltpu.make_async_remote_copy(
            src_ref=chip_sum.at[i, (tp + k) % NZ], dst_ref=rs_in.at[i, k - 1],
            send_sem=rs_s.at[i, k - 1], recv_sem=rs_r.at[i, k - 1], device_id=z_peer(k), device_id_type=MESH)

    def copies_ag(i, k, owner):
        return pltpu.make_async_remote_copy(
            src_ref=gath.at[i, core, owner], dst_ref=gath.at[i, core, owner],
            send_sem=ag_s.at[i, k - 1], recv_sem=ag_r.at[i, k - 1], device_id=z_peer(k), device_id_type=MESH)

    def copies_relay(i, k, side):
        owner = (tp + NZ - k) % NZ
        return pltpu.make_async_remote_copy(
            src_ref=gath.at[i, side, owner], dst_ref=gath.at[i, side, owner],
            send_sem=rl_s.at[i, k], recv_sem=rl_r.at[i, k], device_id=partner, device_id_type=MESH)

    def ar_start(i, partial):
        part[i, 0] = partial[:, :DH]
        part[i, 1] = partial[:, DH:]
        copies_core(i).start()

    def ar_chip(i):
        copies_core(i).wait_recv()
        chip_sum[i] = (part[i, core] + core_in[i]).reshape(NZ, NQ, DH)
        for k in (2, 1, 3):
            copies_rs(i, k).start()

    def ar_own(i, before):
        for k in (1, 2, 3):
            copies_rs(i, k).wait_recv()
        total = chip_sum[i, tp] + rs_in[i, 0] + rs_in[i, 1] + rs_in[i, 2]
        gath[i, core, tp] = (before + total).astype(BF16).astype(F32)
        for k in (2, 1, 3):
            copies_ag(i, k, tp).start()
        copies_relay(i, 0, core).start()

    def ar_relay(i):
        for k in (1, 2, 3):
            copies_ag(i, k, (tp + NZ - k) % NZ).wait_recv()
            copies_relay(i, k, core).start()

    def ar_rows(i):
        for k in range(4):
            copies_relay(i, k, 1 - core).wait_recv()
        return jnp.concatenate([gath[i, 0].reshape(N, DH), gath[i, 1].reshape(N, DH)], axis=1)

    def ar_drain(i):
        copies_core(i).wait_send()
        for k in (1, 2, 3):
            copies_rs(i, k).wait_send()
            copies_ag(i, k, tp).wait_send()
        for k in range(4):
            copies_relay(i, k, core).wait_send()

    first = dot(attn, wob[...])
    for b in range(NB):
        ar_start(b, first[b * N:(b + 1) * N])

    def own_x(b):
        row0 = pl.multiple_of(b * N + tp * NQ, 8)
        return jnp.where(core == 0, xb[pl.ds(row0, NQ), 0:DH].astype(F32), xb[pl.ds(row0, NQ), DH:D].astype(F32))

    def mlp(b):
        rows = ar_rows(b)
        b_t = jnp.transpose(jnp.concatenate([normed(rows, gain(1))] * PK, axis=0)).astype(BF16)
        act_t[...] = b_t
        if b == 0:
            for copy in loads[5:8]:
                copy.wait()
        for j in range(4):
            gate = dot(wgb[j * 256:(j + 1) * 256], act_t[...])
            up = dot(wub[j * 256:(j + 1) * 256], act_t[...])
            u_t = gate * (1.0 / (1.0 + jnp.exp(-gate))) * up
            u_buf[:, j * 256:(j + 1) * 256] = jnp.transpose(u_t).astype(BF16)
        ar_start(NB + b, dot(u_buf[0:N], wdb[...]))

    def own_resid(b):
        return gath[b, core, tp]

    def final_rows(b):
        rows = ar_rows(NB + b)
        return normed(rows, gain(2))

    lane = lax.broadcasted_iota(jnp.int32, (1, TOK), 1)
    group = lane // N
    tgt_row = target[...] - shard * VOC

    M_OWN, S_OWN, M_C, S_C, TGT = 0, 1, 2, 3, 4
    kind = lax.broadcasted_iota(jnp.int32, (8, TOK), 0)
    blank = jnp.where((kind == M_OWN) | (kind == M_C), NEG, 0.0)
    for b in range(NB + 1):
        stat[b] = blank

    def turn(vals, b, j):
        shift = ((b - j) % PK) * N
        return pltpu.roll(vals, shift, 1) if shift else vals

    def packed_targets(b):
        wide = jnp.broadcast_to(tgt_row, (8, TOK))
        packed = wide
        for j in range(PK):
            packed = jnp.where(group == j, turn(wide, j, b), packed)
        return packed[0:1]

    def own_update(z, b, rows, hit_row, lo, hi):
        live = (rows >= lo) & (rows < hi)
        zm = jnp.where(live, z, NEG)
        m_old = stat[b, M_OWN:M_OWN + 1]
        m_new = jnp.maximum(m_old, jnp.max(zm, axis=0, keepdims=True))
        s_add = jnp.sum(jnp.exp(zm - m_new), axis=0, keepdims=True)
        stat[b, S_OWN:S_OWN + 1] = stat[b, S_OWN:S_OWN + 1] * jnp.exp(m_old - m_new) + s_add
        stat[b, M_OWN:M_OWN + 1] = m_new
        hit = live & (rows == hit_row)
        stat[b, TGT:TGT + 1] = stat[b, TGT:TGT + 1] + jnp.sum(jnp.where(hit, z, 0.0), axis=0, keepdims=True)

    def y_copy(b, i):
        return pltpu.make_async_remote_copy(
            src_ref=zsend.at[b, i], dst_ref=zrecv.at[b, i], send_sem=y_s.at[b, i], recv_sem=y_r.at[b, i],
            device_id=across, device_id_type=MESH)

    def next_load(g):
        @pl.when(g + NBUF < (NB + 1) * NCH)
        def _():
            w_load(g + NBUF).start()

    packed_row = lax.broadcasted_iota(jnp.int32, (CP, TOK), 0) + group * CP

    def send(b, start, stop):
        hit_row = packed_targets(b) - send_base

        def send_chunk(i, carry):
            g = b * NCH + i
            w_load(g).wait()
            slot = g % NBUF
            acc = dot(wbuf[slot, 0:CP], hid_t[b])
            for j in range(1, PK):
                acc = jnp.where(group >= j, dot(wbuf[slot, j * CP:(j + 1) * CP], hid_t[b]), acc)
            z = acc * INV_TEMP
            zsend[b, i] = z
            y_copy(b, i).start()
            next_load(g)
            own_update(z, b, packed_row + i * C, hit_row, half * LAP, MID + half * LAP)
            return carry

        lax.fori_loop(start, stop, send_chunk, 0)

    keep_lo = (1 - half) * LAP
    keep_hi = MID + (1 - half) * LAP

    def keep():
        row_id = lax.broadcasted_iota(jnp.int32, (C, TOK), 0)
        hit_row = tgt_row - keep_base
        all_t = hid_t[0]
        for b in range(1, NB):
            all_t = jnp.where(group >= b, hid_t[b], all_t)
        hid_all[...] = all_t

        def keep_chunk(i, carry):
            g = NB * NCH + i
            w_load(g).wait()
            z = dot(wbuf[g % NBUF], hid_all[...]) * INV_TEMP
            zkeep[i] = z
            next_load(g)
            own_update(z, NB, row_id + i * C, hit_row, keep_lo, keep_hi)
            return carry

        lax.fori_loop(0, NCH, keep_chunk, 0)

    def merge():
        for b in range(NB):
            for j in range(PK):
                moved = turn(stat[b], b, j)
                m_in, s_in = moved[M_OWN:M_OWN + 1], moved[S_OWN:S_OWN + 1]
                m_old = stat[NB, M_OWN:M_OWN + 1]
                s_old = stat[NB, S_OWN:S_OWN + 1]
                t_old = stat[NB, TGT:TGT + 1]
                m_new = jnp.maximum(m_old, m_in)
                s_new = s_old * jnp.exp(m_old - m_new) + s_in * jnp.exp(m_in - m_new)
                here = group == b
                stat[NB, M_OWN:M_OWN + 1] = jnp.where(here, m_new, m_old)
                stat[NB, S_OWN:S_OWN + 1] = jnp.where(here, s_new, s_old)
                stat[NB, TGT:TGT + 1] = jnp.where(here, t_old + moved[TGT:TGT + 1], t_old)

    def pair():
        row_cp = lax.broadcasted_iota(jnp.int32, (CP, TOK), 0)

        def pair_chunk(i, carry):
            for b in range(NB):
                y_copy(b, i).wait_recv()
                y_copy(b, i).wait_send()
            for j in range(PK):
                rows = row_cp + (i * C + j * CP)
                live = (rows >= keep_lo) & (rows < keep_hi)
                own = zkeep[i, j * CP:(j + 1) * CP]
                other = turn(zrecv[0, i], 0, j)
                for b in range(1, NB):
                    other = jnp.where(group >= b, turn(zrecv[b, i], b, j), other)
                z0 = jnp.where(pol, own, other)
                diff = jnp.where(pol, own - other, other - own)
                zm = jnp.where(live, z0, NEG)
                m_old = stat[NB, M_C:M_C + 1]
                m_new = jnp.maximum(m_old, jnp.max(zm, axis=0, keepdims=True))
                add = jnp.sum(jnp.exp(zm - m_new) * diff, axis=0, keepdims=True)
                stat[NB, S_C:S_C + 1] = stat[NB, S_C:S_C + 1] * jnp.exp(m_old - m_new) + add
                stat[NB, M_C:M_C + 1] = m_new
            return carry

        lax.fori_loop(0, NCH, pair_chunk, 0)

    def rows_out(b):
        hid_t[b] = jnp.transpose(jnp.concatenate([final_rows(b)] * PK, axis=0)).astype(BF16)

    steps = [
        ar_chip, lambda b: ar_own(b, own_x(b)), ar_relay, mlp,
        lambda b: ar_chip(NB + b), lambda b: ar_own(NB + b, own_resid(b)), lambda b: ar_relay(NB + b), rows_out,
    ]
    for item in ORDER:
        if len(item) == 2:
            steps[item[1]](item[0])
        else:
            send(*item)
    keep()
    for i in range(2 * NB):
        ar_drain(i)
    merge()
    pair()

    def stat_copy(k, slot):
        return pltpu.make_async_remote_copy(
            src_ref=stat.at[NB], dst_ref=stats_in.at[slot], send_sem=f_s.at[k - 1], recv_sem=f_r.at[k - 1],
            device_id=rel_peer(k), device_id_type=MESH)

    for k in range(1, 16):
        stat_copy(k, me).start()
    stats_in[me] = stat[NB]
    for k in range(1, 16):
        stat_copy(k, (me + 16 - k) % 16).wait_recv()

    def lse(model):
        ids = [i for i in range(16) if (i % 4) // 2 == model]
        top = functools.reduce(jnp.maximum, [stats_in[i, M_OWN:M_OWN + 1] for i in ids])
        tot = sum(stats_in[i, S_OWN:S_OWN + 1] * jnp.exp(stats_in[i, M_OWN:M_OWN + 1] - top) for i in ids)
        return top, tot

    top0, tot0 = lse(0)
    top1, tot1 = lse(1)
    lse0, lse1 = top0 + jnp.log(tot0), top1 + jnp.log(tot1)
    cross = sum(stats_in[i, S_C:S_C + 1] * jnp.exp(stats_in[i, M_C:M_C + 1] - top0) for i in range(16))
    tgt_z = sum(stats_in[i, TGT:TGT + 1] for i in range(16) if (i % 4) // 2 == 0)
    out[...] = jnp.concatenate([cross / tot0 - lse0 + lse1, tgt_z - lse0], axis=0)

    for k in range(1, 16):
        stat_copy(k, me).wait_send()


def solution(mesh):
    by_shard = P(("role", "tp"), None)
    by_role = P("role", None)

    def per_device(hidden, segment_ids, loss_mask, target, norm_gains, w_query, b_query, w_key, b_key, w_value, b_value, w_out, w_gate, w_up, w_down, w_head):
        anywhere = pl.BlockSpec(memory_space=pl.ANY)
        vmem = pl.BlockSpec(memory_space=pltpu.VMEM)
        dma = pltpu.SemaphoreType.DMA
        pair = pl.pallas_call(
            kernel,
            out_shape=jax.ShapeDtypeStruct((2, TOK), F32),
            in_specs=[anywhere] * 10 + [vmem] * 5,
            out_specs=vmem,
            scratch_shapes=[
                pltpu.VMEM((TOK, D), BF16),
                pltpu.VMEM((3, 2, D), F32),
                pltpu.VMEM((384, D), BF16),
                pltpu.VMEM((256, D), BF16),
                pltpu.VMEM((FF, D), BF16),
                pltpu.VMEM((FF, D), BF16),
                pltpu.VMEM((FF, D), BF16),
                pltpu.VMEM((NBUF, C, D), BF16),
                pltpu.VMEM((TOK, TOK), F32),
                pltpu.VMEM((D, TOK), BF16),
                pltpu.VMEM((2 * NB, 2, N, DH), F32),
                pltpu.VMEM((2 * NB, N, DH), F32),
                pltpu.VMEM((2 * NB, NZ, NQ, DH), F32),
                pltpu.VMEM((2 * NB, NZ - 1, NQ, DH), F32),
                pltpu.VMEM((2 * NB, 2, NZ, NQ, DH), F32),
                pltpu.VMEM((NB, D, TOK), BF16),
                pltpu.VMEM((D, TOK), BF16),
                pltpu.VMEM((TOK, FF), BF16),
                pltpu.VMEM((NB, NCH, CP, TOK), F32),
                pltpu.VMEM((NB, NCH, CP, TOK), F32),
                pltpu.VMEM((NCH, C, TOK), F32),
                pltpu.VMEM((NB + 1, 8, TOK), F32),
                pltpu.VMEM((16, 8, TOK), F32),
                dma((9,)), dma((NBUF,)),
                dma((2 * NB,)), dma((2 * NB,)),
                dma((2 * NB, 3)), dma((2 * NB, 3)),
                dma((2 * NB, 3)), dma((2 * NB, 3)),
                dma((2 * NB, 4)), dma((2 * NB, 4)),
                dma((NB, NCH)), dma((NB, NCH)),
                dma((15,)), dma((15,)),
            ],
            compiler_params=pltpu.CompilerParams(
                collective_id=0, has_side_effects=True, vmem_limit_bytes=60 * 1024 * 1024),
        )(hidden, w_query, w_key, w_value, w_out, w_gate, w_up, w_down, w_head, jnp.swapaxes(norm_gains, 0, 1),
          segment_ids.reshape(1, TOK), target.reshape(1, TOK), b_query, b_key, b_value)
        found = loss_mask.astype(F32)
        return pair[0] * found, pair[1] * found

    in_specs = (P(None, "dp", None), P("dp"), P("dp"), P("dp"), P(None, None, None), by_shard, by_shard, by_role, by_role, by_role, by_role, by_shard, by_shard, by_shard, by_shard, by_shard)
    return jax.shard_map(per_device, mesh=mesh, in_specs=in_specs, out_specs=(P("dp"), P("dp")), check_vma=False)
```

```python
import functools
import math

import jax
import jax.numpy as jnp
from jax import lax
from jax.experimental import pallas as pl
from jax.experimental.pallas import tpu as pltpu
from jax.sharding import PartitionSpec as P

MESH = pl.DeviceIdType.MESH
F32 = jnp.float32
BF16 = jnp.bfloat16
EPS = 1e-6
LOG_BASE = math.log(1000000.0)
INV_TEMP = 1.0 / 0.7

TOK = 128
D = 2048
DH = D // 2
HEAD = 64
QH = 4
FF = 1024
VOC = 16032
MID = VOC // 2
C = 576
NCH = 14
BLK = C * NCH
OFF = VOC - BLK
LAP = BLK - MID
NBUF = 4
NB = 4
N = TOK // NB
GROUPS = ((0, 32, 4), (32, 32, 4), (64, 64, 2))
NG = len(GROUPS)
QR = C // 4
NZ = 4
NH = N // 2
NEG = -1e30
ORDER = (
    (0, 0), (0, 1), (0, 2), (1, 0), (0, 3), (0, 4), (0, 5), (1, 1), (0, 6), (0, 7),
    (0, 0, 1), (2, 0), (1, 2), (0, 1, 3), (1, 3), (0, 3, 5), (1, 4), (2, 1), (0, 5, 10), (1, 5), (3, 0), (0, 10, 12), (2, 2),
    (0, 12, 14), (2, 3), (1, 6), (3, 1), (1, 7),
    (1, 0, 2), (2, 4), (1, 2, 4), (3, 2), (1, 4, 6), (3, 3), (2, 5), (1, 6, 8), (3, 4), (1, 8, 12), (2, 6), (3, 5), (2, 7),
    (1, 12, 14), (3, 6), (3, 7), (2, 0, 14),
)


def dot(lhs, rhs):
    return jnp.dot(lhs, rhs, preferred_element_type=F32)


def kernel(hid, wq, wk, wv, wo, wg, wu, wd, wh, gains, seg, target, bq, bk, bv,
           out,
           xb, gain_in, wqkv, wob, wgb, wub, wdb, wbuf, tr, act_t, part, core_in, chip_sum, rs_in, gath, hid_t, hid_all, h_rows,
           u_buf, zsend, zrecv, zkeep, stat, stats_in,
           in_sem, w_sem, d_s, d_r, rs_s, rs_r, ag_s, ag_r, rl_s, rl_r, y_s, y_r, f_s, f_r):
    dp, tp, ro = lax.axis_index("dp"), lax.axis_index("tp"), lax.axis_index("role")
    half, core = ro // 2, ro % 2
    shard = core * NZ + tp
    me = tp * 4 + ro
    pol = half == 0
    partner = (dp, tp, ro + 1 - 2 * core)
    across = (dp, tp, (ro + 2) % 4)

    def z_peer(k):
        return (dp, (tp + k) % NZ, ro)

    def rel_peer(k):
        other = (me + k) % 16
        return (dp, other // 4, other % 4)

    loads = [
        pltpu.make_async_copy(hid.at[half], xb, in_sem.at[0]),
        pltpu.make_async_copy(wq, wqkv.at[pl.ds(0, 256)], in_sem.at[1]),
        pltpu.make_async_copy(wk.at[pl.ds(pl.multiple_of(tp * HEAD, HEAD), HEAD)], wqkv.at[pl.ds(256, HEAD)], in_sem.at[2]),
        pltpu.make_async_copy(wv.at[pl.ds(pl.multiple_of(tp * HEAD, HEAD), HEAD)], wqkv.at[pl.ds(320, HEAD)], in_sem.at[3]),
        pltpu.make_async_copy(wo, wob, in_sem.at[4]),
        pltpu.make_async_copy(wg, wgb, in_sem.at[5]),
        pltpu.make_async_copy(wu, wub, in_sem.at[6]),
        pltpu.make_async_copy(wd, wdb, in_sem.at[7]),
        pltpu.make_async_copy(gains, gain_in, in_sem.at[8]),
    ]
    first_loads = loads[0:4] + loads[8:9]
    for copy in first_loads:
        copy.start()

    barrier = pltpu.get_barrier_semaphore()
    for k in range(1, 16):
        pl.semaphore_signal(barrier, inc=1, device_id=rel_peer(k), device_id_type=MESH)

    send_base = half * OFF
    keep_base = (1 - half) * OFF

    def w_load(g):
        kept = g // NCH >= NG
        base = jnp.where(kept, keep_base, send_base) + (g % NCH) * C
        slot = g % NBUF
        return pltpu.make_async_copy(wh.at[pl.ds(pl.multiple_of(base, 16), C)], wbuf.at[slot], w_sem.at[slot])

    rows8 = lax.broadcasted_iota(jnp.int32, (QH, HEAD), 0)
    tr[...] = jnp.zeros_like(tr)
    tr[0:QH, 0:HEAD] = bq[...].astype(F32)
    pick = rows8 == tp
    tr[QH:QH + 1, 0:HEAD] = jnp.sum(jnp.where(pick, bk[...].astype(F32), 0.0), axis=0, keepdims=True)
    tr[QH + 1:QH + 2, 0:HEAD] = jnp.sum(jnp.where(pick, bv[...].astype(F32), 0.0), axis=0, keepdims=True)
    seg_row = seg[...].astype(F32)
    tr[QH + 2:QH + 3, :] = seg_row
    cols = jnp.transpose(tr[...])
    seg_col = cols[:, QH + 2:QH + 3]
    src_id = lax.broadcasted_iota(jnp.int32, (TOK, TOK), 0)
    dst_id = lax.broadcasted_iota(jnp.int32, (TOK, TOK), 1)
    allowed = (seg_col == seg_row) & (src_id <= dst_id)
    pos = jnp.sum(jnp.where(allowed, 1.0, 0.0), axis=0, keepdims=True) - 1.0
    rot_id = lax.broadcasted_iota(jnp.int32, (HEAD // 2, TOK), 0).astype(F32)
    angles = pos * jnp.exp(rot_id * (-2.0 * LOG_BASE / HEAD))
    cos_part, sin_part = jnp.cos(angles), jnp.sin(angles)

    def normed(rows, scale):
        inv = lax.rsqrt(jnp.mean(rows * rows, axis=-1, keepdims=True) + EPS)
        return rows * inv * scale

    loads[0].wait()
    loads[8].wait()

    def gain(k):
        return jnp.where(pol, gain_in[k, 0:1], gain_in[k, 1:2])

    act_t[...] = jnp.transpose(normed(xb[...].astype(F32), gain(0))).astype(BF16)
    for copy in loads[1:4]:
        copy.wait()
    for copy in loads[4:8]:
        copy.start()
    for g in range(NBUF):
        w_load(g).start()
    qkv = dot(wqkv[...], act_t[...])

    def rotate(vals):
        lo, hi = vals[:HEAD // 2], vals[HEAD // 2:]
        return jnp.concatenate([lo * cos_part - hi * sin_part, hi * cos_part + lo * sin_part], axis=0)

    queries = []
    for h in range(QH):
        q_h = qkv[h * HEAD:(h + 1) * HEAD] + cols[0:HEAD, h:h + 1]
        queries.append(rotate(q_h).astype(BF16))
    q_cat = jnp.concatenate(queries, axis=1)
    key = jnp.transpose(rotate(qkv[256:320] + cols[0:HEAD, QH:QH + 1])).astype(BF16)
    val_t = (qkv[320:384] + cols[0:HEAD, QH + 1:QH + 2]).astype(BF16)
    scores = dot(key, q_cat) * (HEAD ** -0.5)
    scores = jnp.where(jnp.concatenate([allowed] * QH, axis=1), scores, NEG)
    weights = jnp.exp(scores - jnp.max(scores, axis=0, keepdims=True))
    probs = (weights / jnp.sum(weights, axis=0, keepdims=True)).astype(BF16)
    out_t = dot(val_t, probs)
    attn = jnp.transpose(jnp.concatenate([out_t[:, h * TOK:(h + 1) * TOK] for h in range(QH)], axis=0)).astype(BF16)
    loads[4].wait()
    pl.semaphore_wait(barrier, 15)

    mid = (tp == 1) | (tp == 2)
    near = tp // 2
    far = 1 - near

    def copies_core(i):
        return pltpu.make_async_remote_copy(
            src_ref=part.at[i, 1 - core], dst_ref=core_in.at[i], send_sem=d_s.at[i], recv_sem=d_r.at[i],
            device_id=partner, device_id_type=MESH)

    def copies_rs(i, o, slot):
        return pltpu.make_async_remote_copy(
            src_ref=chip_sum.at[i, o], dst_ref=rs_in.at[i, slot],
            send_sem=rs_s.at[i, o], recv_sem=rs_r.at[i, slot], device_id=(dp, 1 + o, ro), device_id_type=MESH)

    def copies_ag(i, o, k):
        return pltpu.make_async_remote_copy(
            src_ref=gath.at[i, core, o], dst_ref=gath.at[i, core, o],
            send_sem=ag_s.at[i, k - 1], recv_sem=ag_r.at[i, o], device_id=z_peer(k), device_id_type=MESH)

    def copies_relay(i, side, o):
        return pltpu.make_async_remote_copy(
            src_ref=gath.at[i, side, o], dst_ref=gath.at[i, side, o],
            send_sem=rl_s.at[i, o], recv_sem=rl_r.at[i, o], device_id=partner, device_id_type=MESH)

    def ar_start(i, partial):
        part[i, 0] = partial[:, :DH]
        part[i, 1] = partial[:, DH:]
        copies_core(i).start()

    def ar_chip(i):
        copies_core(i).wait_recv()
        chip_sum[i] = (part[i, core] + core_in[i]).reshape(2, NH, DH)
        copies_rs(i, far, jnp.where(tp < 1 + far, tp, tp - 1)).start()

        @pl.when(jnp.logical_not(mid))
        def _():
            copies_rs(i, near, jnp.where(tp < 1 + near, tp, tp - 1)).start()

    def ar_own(i, before):
        @pl.when(mid)
        def _():
            for k in range(3):
                copies_rs(i, near, k).wait_recv()
            total = chip_sum[i, near] + rs_in[i, 0] + rs_in[i, 1] + rs_in[i, 2]
            gath[i, core, near] = (before() + total).astype(BF16).astype(F32)
            for k in (2, 1, 3):
                copies_ag(i, near, k).start()
            copies_relay(i, core, near).start()

    def ar_relay(i):
        @pl.when(jnp.logical_not(mid))
        def _():
            copies_ag(i, near, 1).wait_recv()
            copies_relay(i, core, near).start()

        copies_ag(i, far, 1).wait_recv()
        copies_relay(i, core, far).start()

    def ar_rows(i):
        for o in range(2):
            copies_relay(i, 1 - core, o).wait_recv()
        return jnp.concatenate([gath[i, 0].reshape(N, DH), gath[i, 1].reshape(N, DH)], axis=1)

    def ar_drain(i):
        copies_core(i).wait_send()
        copies_rs(i, far, 0).wait_send()

        @pl.when(jnp.logical_not(mid))
        def _():
            copies_rs(i, near, 0).wait_send()

        @pl.when(mid)
        def _():
            for k in (1, 2, 3):
                copies_ag(i, near, k).wait_send()

        for o in range(2):
            copies_relay(i, core, o).wait_send()

    first = dot(attn, wob[...])
    for b in range(NB):
        ar_start(b, first[b * N:(b + 1) * N])

    def own_x(b):
        row0 = pl.multiple_of(b * N + near * NH, 8)
        return jnp.where(core == 0, xb[pl.ds(row0, NH), 0:DH].astype(F32), xb[pl.ds(row0, NH), DH:D].astype(F32))

    def mlp(b):
        rows = ar_rows(b)
        b_t = jnp.transpose(jnp.concatenate([normed(rows, gain(1))] * (TOK // N), axis=0)).astype(BF16)
        act_t[...] = b_t
        if b == 0:
            for copy in loads[5:8]:
                copy.wait()
        for j in range(4):
            gate = dot(wgb[j * 256:(j + 1) * 256], act_t[...])
            up = dot(wub[j * 256:(j + 1) * 256], act_t[...])
            u_t = gate * (1.0 / (1.0 + jnp.exp(-gate))) * up
            u_buf[:, j * 256:(j + 1) * 256] = jnp.transpose(u_t).astype(BF16)
        ar_start(NB + b, dot(u_buf[0:N], wdb[...]))

    def own_resid(b):
        return gath[b, core, near]

    def final_rows(b):
        rows = ar_rows(NB + b)
        return normed(rows, gain(2))

    lane = lax.broadcasted_iota(jnp.int32, (1, TOK), 1)
    tgt_row = target[...] - shard * VOC

    M_OWN, S_OWN, M_C, S_C, TGT = 0, 1, 2, 3, 4
    kind = lax.broadcasted_iota(jnp.int32, (8, TOK), 0)
    blank = jnp.where((kind == M_OWN) | (kind == M_C), NEG, 0.0)
    for e in range(NG + 1):
        stat[e] = blank

    def inside(e):
        first_tok, size, _ = GROUPS[e]
        return (lane >= first_tok) & (lane < first_tok + size)

    def turn(vals, e, j, back=False):
        shift = GROUPS[e][0] - j * GROUPS[e][1]
        shift = (-shift if back else shift) % TOK
        return pltpu.roll(vals, shift, 1) if shift else vals

    def packed_targets(e):
        wide = jnp.broadcast_to(tgt_row, (8, TOK))
        packed = turn(wide, e, 0, True)
        for j in range(1, GROUPS[e][2]):
            packed = jnp.where(lane >= j * GROUPS[e][1], turn(wide, e, j, True), packed)
        return packed[0:1]

    def own_update(z, b, rows, hit_row, lo, hi):
        live = (rows >= lo) & (rows < hi)
        zm = jnp.where(live, z, NEG)
        m_old = stat[b, M_OWN:M_OWN + 1]
        m_new = jnp.maximum(m_old, jnp.max(zm, axis=0, keepdims=True))
        s_add = jnp.sum(jnp.exp(zm - m_new), axis=0, keepdims=True)
        stat[b, S_OWN:S_OWN + 1] = stat[b, S_OWN:S_OWN + 1] * jnp.exp(m_old - m_new) + s_add
        stat[b, M_OWN:M_OWN + 1] = m_new
        hit = live & (rows == hit_row)
        stat[b, TGT:TGT + 1] = stat[b, TGT:TGT + 1] + jnp.sum(jnp.where(hit, z, 0.0), axis=0, keepdims=True)

    def packed_rows(e, i):
        rows = C // GROUPS[e][2]
        start = NCH * C * GROUPS[e][0] // TOK + i * rows
        return pl.ds(pl.multiple_of(start, 8), rows)

    def y_copy(e, i):
        where = packed_rows(e, i)
        return pltpu.make_async_remote_copy(
            src_ref=zsend.at[where], dst_ref=zrecv.at[where], send_sem=y_s.at[e, i], recv_sem=y_r.at[e, i],
            device_id=across, device_id_type=MESH)

    def next_load(g):
        @pl.when(g + NBUF < (NG + 1) * NCH)
        def _():
            w_load(g + NBUF).start()

    def send(e, start, stop):
        _, size, wide = GROUPS[e]
        rows = C // wide
        hit_row = packed_targets(e) - send_base
        packed_row = lax.broadcasted_iota(jnp.int32, (rows, TOK), 0) + lane // size * rows

        def send_chunk(i, carry):
            g = e * NCH + i
            w_load(g).wait()
            slot = g % NBUF
            acc = dot(wbuf[slot, 0:rows], hid_t[e])
            for j in range(1, wide):
                acc = jnp.where(lane >= j * size, dot(wbuf[slot, j * rows:(j + 1) * rows], hid_t[e]), acc)
            z = acc * INV_TEMP
            zsend[packed_rows(e, i)] = z
            y_copy(e, i).start()
            next_load(g)
            own_update(z, e, packed_row + i * C, hit_row, half * LAP, MID + half * LAP)
            return carry

        lax.fori_loop(start, stop, send_chunk, 0)

    keep_lo = (1 - half) * LAP
    keep_hi = MID + (1 - half) * LAP

    def keep():
        row_id = lax.broadcasted_iota(jnp.int32, (C, TOK), 0)
        hit_row = tgt_row - keep_base
        all_t = hid_t[0]
        for e in range(1, NG):
            all_t = jnp.where(lane >= GROUPS[e][0], hid_t[e], all_t)
        hid_all[...] = all_t

        def keep_chunk(i, carry):
            g = NG * NCH + i
            w_load(g).wait()
            z = dot(wbuf[g % NBUF], hid_all[...]) * INV_TEMP
            zkeep[i] = z
            next_load(g)
            own_update(z, NG, row_id + i * C, hit_row, keep_lo, keep_hi)
            return carry

        lax.fori_loop(0, NCH, keep_chunk, 0)

    def merge():
        for e in range(NG):
            for j in range(GROUPS[e][2]):
                moved = turn(stat[e], e, j)
                m_in, s_in = moved[M_OWN:M_OWN + 1], moved[S_OWN:S_OWN + 1]
                m_old = stat[NG, M_OWN:M_OWN + 1]
                s_old = stat[NG, S_OWN:S_OWN + 1]
                t_old = stat[NG, TGT:TGT + 1]
                m_new = jnp.maximum(m_old, m_in)
                s_new = s_old * jnp.exp(m_old - m_new) + s_in * jnp.exp(m_in - m_new)
                here = inside(e)
                stat[NG, M_OWN:M_OWN + 1] = jnp.where(here, m_new, m_old)
                stat[NG, S_OWN:S_OWN + 1] = jnp.where(here, s_new, s_old)
                stat[NG, TGT:TGT + 1] = jnp.where(here, t_old + moved[TGT:TGT + 1], t_old)

    def pair():
        row_q = lax.broadcasted_iota(jnp.int32, (QR, TOK), 0)

        def section(e, i, q):
            rows = C // GROUPS[e][2]
            start = NCH * C * GROUPS[e][0] // TOK + i * rows + q * QR % rows
            return turn(zrecv[pl.ds(pl.multiple_of(start, 8), QR)], e, q * QR // rows)

        def pair_chunk(i, carry):
            for e in range(NG):
                y_copy(e, i).wait_recv()
                y_copy(e, i).wait_send()
            for q in range(C // QR):
                rows = row_q + (i * C + q * QR)
                live = (rows >= keep_lo) & (rows < keep_hi)
                own = zkeep[i, q * QR:(q + 1) * QR]
                other = section(0, i, q)
                for e in range(1, NG):
                    other = jnp.where(lane >= GROUPS[e][0], section(e, i, q), other)
                z0 = jnp.where(pol, own, other)
                diff = jnp.where(pol, own - other, other - own)
                zm = jnp.where(live, z0, NEG)
                m_old = stat[NG, M_C:M_C + 1]
                m_new = jnp.maximum(m_old, jnp.max(zm, axis=0, keepdims=True))
                add = jnp.sum(jnp.exp(zm - m_new) * diff, axis=0, keepdims=True)
                stat[NG, S_C:S_C + 1] = stat[NG, S_C:S_C + 1] * jnp.exp(m_old - m_new) + add
                stat[NG, M_C:M_C + 1] = m_new
            return carry

        lax.fori_loop(0, NCH, pair_chunk, 0)

    def rows_out(b):
        rows = final_rows(b)
        if b < 2:
            hid_t[b] = jnp.transpose(jnp.concatenate([rows] * 4, axis=0)).astype(BF16)
        elif b == 2:
            h_rows[...] = rows
        else:
            hid_t[2] = jnp.transpose(jnp.concatenate([h_rows[...], rows] * 2, axis=0)).astype(BF16)

    steps = [
        ar_chip, lambda b: ar_own(b, lambda: own_x(b)), ar_relay, mlp,
        lambda b: ar_chip(NB + b), lambda b: ar_own(NB + b, lambda: own_resid(b)), lambda b: ar_relay(NB + b), rows_out,
    ]
    for item in ORDER:
        if len(item) == 2:
            steps[item[1]](item[0])
        else:
            send(*item)
    keep()
    for i in range(2 * NB):
        ar_drain(i)
    merge()
    pair()

    def stat_copy(k, slot):
        return pltpu.make_async_remote_copy(
            src_ref=stat.at[NG], dst_ref=stats_in.at[slot], send_sem=f_s.at[k - 1], recv_sem=f_r.at[k - 1],
            device_id=rel_peer(k), device_id_type=MESH)

    for k in range(1, 16):
        stat_copy(k, me).start()
    stats_in[me] = stat[NG]
    for k in range(1, 16):
        stat_copy(k, (me + 16 - k) % 16).wait_recv()

    def lse(model):
        ids = [i for i in range(16) if (i % 4) // 2 == model]
        top = functools.reduce(jnp.maximum, [stats_in[i, M_OWN:M_OWN + 1] for i in ids])
        tot = sum(stats_in[i, S_OWN:S_OWN + 1] * jnp.exp(stats_in[i, M_OWN:M_OWN + 1] - top) for i in ids)
        return top, tot

    top0, tot0 = lse(0)
    top1, tot1 = lse(1)
    lse0, lse1 = top0 + jnp.log(tot0), top1 + jnp.log(tot1)
    cross = sum(stats_in[i, S_C:S_C + 1] * jnp.exp(stats_in[i, M_C:M_C + 1] - top0) for i in range(16))
    tgt_z = sum(stats_in[i, TGT:TGT + 1] for i in range(16) if (i % 4) // 2 == 0)
    out[...] = jnp.concatenate([cross / tot0 - lse0 + lse1, tgt_z - lse0], axis=0)

    for k in range(1, 16):
        stat_copy(k, me).wait_send()


def solution(mesh):
    by_shard = P(("role", "tp"), None)
    by_role = P("role", None)

    def per_device(hidden, segment_ids, loss_mask, target, norm_gains, w_query, b_query, w_key, b_key, w_value, b_value, w_out, w_gate, w_up, w_down, w_head):
        anywhere = pl.BlockSpec(memory_space=pl.ANY)
        vmem = pl.BlockSpec(memory_space=pltpu.VMEM)
        dma = pltpu.SemaphoreType.DMA
        pair = pl.pallas_call(
            kernel,
            out_shape=jax.ShapeDtypeStruct((2, TOK), F32),
            in_specs=[anywhere] * 10 + [vmem] * 5,
            out_specs=vmem,
            scratch_shapes=[
                pltpu.VMEM((TOK, D), BF16),
                pltpu.VMEM((3, 2, D), F32),
                pltpu.VMEM((384, D), BF16),
                pltpu.VMEM((256, D), BF16),
                pltpu.VMEM((FF, D), BF16),
                pltpu.VMEM((FF, D), BF16),
                pltpu.VMEM((FF, D), BF16),
                pltpu.VMEM((NBUF, C, D), BF16),
                pltpu.VMEM((TOK, TOK), F32),
                pltpu.VMEM((D, TOK), BF16),
                pltpu.VMEM((2 * NB, 2, N, DH), F32),
                pltpu.VMEM((2 * NB, N, DH), F32),
                pltpu.VMEM((2 * NB, 2, NH, DH), F32),
                pltpu.VMEM((2 * NB, 3, NH, DH), F32),
                pltpu.VMEM((2 * NB, 2, 2, NH, DH), F32),
                pltpu.VMEM((NG, D, TOK), BF16),
                pltpu.VMEM((D, TOK), BF16),
                pltpu.VMEM((N, D), F32),
                pltpu.VMEM((TOK, FF), BF16),
                pltpu.VMEM((BLK, TOK), F32),
                pltpu.VMEM((BLK, TOK), F32),
                pltpu.VMEM((NCH, C, TOK), F32),
                pltpu.VMEM((NG + 1, 8, TOK), F32),
                pltpu.VMEM((16, 8, TOK), F32),
                dma((9,)), dma((NBUF,)),
                dma((2 * NB,)), dma((2 * NB,)),
                dma((2 * NB, 2)), dma((2 * NB, 3)),
                dma((2 * NB, 3)), dma((2 * NB, 2)),
                dma((2 * NB, 2)), dma((2 * NB, 2)),
                dma((NG, NCH)), dma((NG, NCH)),
                dma((15,)), dma((15,)),
            ],
            compiler_params=pltpu.CompilerParams(
                collective_id=0, has_side_effects=True, vmem_limit_bytes=60 * 1024 * 1024),
        )(hidden, w_query, w_key, w_value, w_out, w_gate, w_up, w_down, w_head, jnp.swapaxes(norm_gains, 0, 1),
          segment_ids.reshape(1, TOK), target.reshape(1, TOK), b_query, b_key, b_value)
        found = loss_mask.astype(F32)
        return pair[0] * found, pair[1] * found

    in_specs = (P(None, "dp", None), P("dp"), P("dp"), P("dp"), P(None, None, None), by_shard, by_shard, by_role, by_role, by_role, by_role, by_shard, by_shard, by_shard, by_shard, by_shard)
    return jax.shard_map(per_device, mesh=mesh, in_specs=in_specs, out_specs=(P("dp"), P("dp")), check_vma=False)
```

```python
import functools
import math

import jax
import jax.numpy as jnp
from jax import lax
from jax.experimental import pallas as pl
from jax.experimental.pallas import tpu as pltpu
from jax.sharding import PartitionSpec as P

MESH = pl.DeviceIdType.MESH
F32 = jnp.float32
BF16 = jnp.bfloat16
EPS = 1e-6
LOG_BASE = math.log(1000000.0)
INV_TEMP = 1.0 / 0.7

TOK = 128
D = 2048
DH = D // 2
HEAD = 64
QH = 4
FF = 1024
VOC = 16032
MID = VOC // 2
C = 576
NCH = 14
BLK = C * NCH
OFF = VOC - BLK
LAP = BLK - MID
NBUF = 4
NB = 4
N = TOK // NB
GROUPS = ((0, 32, 4), (32, 32, 4), (64, 32, 4), (96, 32, 4))
NG = len(GROUPS)
QR = C // 4
NZ = 4
NH = N // 2
PR = NH // 2
NEG = -1e30
ORDER = (
    "a0,x,a1,a2,b0,a3,a4,a5,a6,b1,a7",
    "A2,c0,A1,b2,A1,b3,A2,b4,c1,A6,b5,A2,c2,b6,d0,b7",
    "B2,c3,d1,B2,c4,B4,d2,B2,c5,d3,B2,d4,c6,B2,c7",
    "C4,d5,C4,d6,C2,d7,C4,D14",
)


def dot(lhs, rhs):
    return jnp.dot(lhs, rhs, preferred_element_type=F32)


def kernel(hid, wq, wk, wv, wo, wg, wu, wd, wh, gains, seg, target, bq, bk, bv,
           out,
           xb, gain_in, wqkv, wob, wgb, wub, wdb, wbuf, tr, act_t, part, core_in, chip_sum, rs_in, gath, hid_t, hid_all,
           u_buf, zsend, zrecv, zkeep, stat, own_shares, own_in, cross_shares, cross_in,
           in_sem, w_sem, ar_s, d_r, rs_r, ag_r, rl_r, y_s, y_r, f_s, f_r):
    dp, tp, ro = lax.axis_index("dp"), lax.axis_index("tp"), lax.axis_index("role")
    half, core = ro // 2, ro % 2
    shard = core * NZ + tp
    me = tp * 4 + ro
    pol = half == 0
    partner = (dp, tp, ro + 1 - 2 * core)
    across = (dp, tp, (ro + 2) % 4)

    def z_peer(k):
        return (dp, (tp + k) % NZ, ro)

    def rel_peer(k):
        other = (me + k) % 16
        return (dp, other // 4, other % 4)

    loads = [
        pltpu.make_async_copy(hid.at[half], xb, in_sem.at[0]),
        pltpu.make_async_copy(wq, wqkv.at[pl.ds(0, 256)], in_sem.at[1]),
        pltpu.make_async_copy(wk.at[pl.ds(pl.multiple_of(tp * HEAD, HEAD), HEAD)], wqkv.at[pl.ds(256, HEAD)], in_sem.at[2]),
        pltpu.make_async_copy(wv.at[pl.ds(pl.multiple_of(tp * HEAD, HEAD), HEAD)], wqkv.at[pl.ds(320, HEAD)], in_sem.at[3]),
        pltpu.make_async_copy(wo, wob, in_sem.at[4]),
        pltpu.make_async_copy(wg, wgb, in_sem.at[5]),
        pltpu.make_async_copy(wu, wub, in_sem.at[6]),
        pltpu.make_async_copy(wd, wdb, in_sem.at[7]),
        pltpu.make_async_copy(gains, gain_in, in_sem.at[8]),
    ]
    first_loads = loads[0:4] + loads[8:9]
    for copy in first_loads:
        copy.start()

    barrier = pltpu.get_barrier_semaphore()
    for k in range(1, 16):
        pl.semaphore_signal(barrier, inc=1, device_id=rel_peer(k), device_id_type=MESH)

    send_base = half * OFF
    keep_base = (1 - half) * OFF

    def w_load(g):
        kept = g // NCH >= NG
        base = jnp.where(kept, keep_base, send_base) + (g % NCH) * C
        slot = g % NBUF
        return pltpu.make_async_copy(wh.at[pl.ds(pl.multiple_of(base, 16), C)], wbuf.at[slot], w_sem.at[slot])

    rows8 = lax.broadcasted_iota(jnp.int32, (QH, HEAD), 0)
    tr[...] = jnp.zeros_like(tr)
    tr[0:QH, 0:HEAD] = bq[...].astype(F32)
    pick = rows8 == tp
    tr[QH:QH + 1, 0:HEAD] = jnp.sum(jnp.where(pick, bk[...].astype(F32), 0.0), axis=0, keepdims=True)
    tr[QH + 1:QH + 2, 0:HEAD] = jnp.sum(jnp.where(pick, bv[...].astype(F32), 0.0), axis=0, keepdims=True)
    seg_row = seg[...].astype(F32)
    tr[QH + 2:QH + 3, :] = seg_row
    cols = jnp.transpose(tr[...])
    seg_col = cols[:, QH + 2:QH + 3]
    src_id = lax.broadcasted_iota(jnp.int32, (TOK, TOK), 0)
    dst_id = lax.broadcasted_iota(jnp.int32, (TOK, TOK), 1)
    allowed = (seg_col == seg_row) & (src_id <= dst_id)
    pos = jnp.sum(jnp.where(allowed, 1.0, 0.0), axis=0, keepdims=True) - 1.0
    rot_id = lax.broadcasted_iota(jnp.int32, (HEAD // 2, TOK), 0).astype(F32)
    angles = pos * jnp.exp(rot_id * (-2.0 * LOG_BASE / HEAD))
    cos_part, sin_part = jnp.cos(angles), jnp.sin(angles)

    def normed(rows, scale):
        inv = lax.rsqrt(jnp.mean(rows * rows, axis=-1, keepdims=True) + EPS)
        return rows * inv * scale

    loads[0].wait()
    loads[8].wait()

    def gain(k):
        return jnp.where(pol, gain_in[k, 0:1], gain_in[k, 1:2])

    def rotate(vals, n):
        lo, hi = vals[:HEAD // 2], vals[HEAD // 2:]
        cos_n, sin_n = cos_part[:, :n], sin_part[:, :n]
        return jnp.concatenate([lo * cos_n - hi * sin_n, hi * cos_n + lo * sin_n], axis=0)

    def attention(n):
        rows_t = jnp.transpose(normed(xb[0:n].astype(F32), gain(0))).astype(BF16)
        qkv = dot(wqkv[...], rows_t)
        key = jnp.transpose(rotate(qkv[256:320] + cols[0:HEAD, QH:QH + 1], n)).astype(BF16)
        val_t = (qkv[320:384] + cols[0:HEAD, QH + 1:QH + 2]).astype(BF16)
        outs = []
        for h in range(QH):
            query = rotate(qkv[h * HEAD:(h + 1) * HEAD] + cols[0:HEAD, h:h + 1], n).astype(BF16)
            scores = jnp.where(allowed[0:n, 0:n], dot(key, query) * (HEAD ** -0.5), NEG)
            weights = jnp.exp(scores - jnp.max(scores, axis=0, keepdims=True))
            probs = (weights / jnp.sum(weights, axis=0, keepdims=True)).astype(BF16)
            outs.append(dot(val_t, probs))
        return jnp.transpose(jnp.concatenate(outs, axis=0)).astype(BF16)

    for copy in loads[1:4]:
        copy.wait()
    for copy in loads[4:8]:
        copy.start()
    for g in range(NBUF):
        w_load(g).start()
    attn = attention(N)
    loads[4].wait()
    pl.semaphore_wait(barrier, 15)

    mid = (tp == 1) | (tp == 2)
    near = tp // 2
    far = 1 - near

    def copies_core(i):
        return pltpu.make_async_remote_copy(
            src_ref=part.at[i, 1 - core], dst_ref=core_in.at[i], send_sem=ar_s.at[i], recv_sem=d_r.at[i],
            device_id=partner, device_id_type=MESH)

    def copies_rs(i, o, slot, p):
        return pltpu.make_async_remote_copy(
            src_ref=chip_sum.at[i, o, p], dst_ref=rs_in.at[i, p, slot], send_sem=ar_s.at[i],
            recv_sem=rs_r.at[i, p], device_id=(dp, 1 + o, ro), device_id_type=MESH)

    def copies_ag(i, o, k, p):
        return pltpu.make_async_remote_copy(
            src_ref=gath.at[i, core, o, p], dst_ref=gath.at[i, core, o, p], send_sem=ar_s.at[i],
            recv_sem=ag_r.at[i, 2 * o + p], device_id=z_peer(k), device_id_type=MESH)

    def copies_relay(i, side, o, p):
        return pltpu.make_async_remote_copy(
            src_ref=gath.at[i, side, o, p], dst_ref=gath.at[i, side, o, p],
            send_sem=ar_s.at[i], recv_sem=rl_r.at[i], device_id=partner, device_id_type=MESH)

    def all_of(ref, send_sem, recv_sem):
        return pltpu.make_async_remote_copy(
            src_ref=ref, dst_ref=ref, send_sem=send_sem, recv_sem=recv_sem, device_id=partner, device_id_type=MESH)

    def ar_start(i, lhs, w_ref):
        theirs = pl.ds(pl.multiple_of((1 - core) * DH, DH), DH)
        ours = pl.ds(pl.multiple_of(core * DH, DH), DH)
        part[i, 1 - core] = dot(lhs, w_ref[:, theirs])
        copies_core(i).start()
        part[i, core] = dot(lhs, w_ref[:, ours])

    def ar_chip(i):
        copies_core(i).wait_recv()
        chip_sum[i] = (part[i, core] + core_in[i]).reshape(2, 2, PR, DH)
        for p in range(2):
            copies_rs(i, far, jnp.where(tp < 1 + far, tp, tp - 1), p).start()

            @pl.when(jnp.logical_not(mid))
            def _():
                copies_rs(i, near, jnp.where(tp < 1 + near, tp, tp - 1), p).start()

    def ar_own(i, before):
        @pl.when(mid)
        def _():
            for p in range(2):
                all_of(rs_in.at[i, p], ar_s.at[i], rs_r.at[i, p]).wait_recv()
                total = chip_sum[i, near, p] + rs_in[i, p, 0] + rs_in[i, p, 1] + rs_in[i, p, 2]
                gath[i, core, near, p] = (before(p) + total).astype(BF16).astype(F32)
                for k in (2, 1, 3):
                    copies_ag(i, near, k, p).start()
                copies_relay(i, core, near, p).start()

    def ar_relay(i):
        for p in range(2):
            @pl.when(jnp.logical_not(mid))
            def _():
                copies_ag(i, near, 1, p).wait_recv()
                copies_relay(i, core, near, p).start()

            copies_ag(i, far, 1, p).wait_recv()
            copies_relay(i, core, far, p).start()

    def ar_rows(i):
        all_of(gath.at[i, 1 - core], ar_s.at[i], rl_r.at[i]).wait_recv()
        return jnp.concatenate([gath[i, 0].reshape(N, DH), gath[i, 1].reshape(N, DH)], axis=1)

    def ar_drain(i):
        @pl.when(mid)
        def _():
            all_of(gath.at[pl.ds(0, 2)], ar_s.at[i], rl_r.at[i]).wait_send()

        @pl.when(jnp.logical_not(mid))
        def _():
            all_of(rs_in.at[pl.ds(0, 2)], ar_s.at[i], rl_r.at[i]).wait_send()

    ar_start(0, attn, wob)

    def attend_rest():
        heads = attention(TOK)
        for b in range(1, NB):
            ar_start(b, heads[b * N:(b + 1) * N], wob)

    def own_x(b, p):
        rows = pl.ds(pl.multiple_of(b * N + near * NH + p * PR, 8), PR)
        return jnp.where(core == 0, xb[rows, 0:DH].astype(F32), xb[rows, DH:D].astype(F32))

    def mlp(b):
        rows = ar_rows(b)
        b_t = jnp.transpose(jnp.concatenate([normed(rows, gain(1))] * (TOK // N), axis=0)).astype(BF16)
        act_t[...] = b_t
        if b == 0:
            for copy in loads[5:8]:
                copy.wait()
        for j in range(4):
            gate = dot(wgb[j * 256:(j + 1) * 256], act_t[...])
            up = dot(wub[j * 256:(j + 1) * 256], act_t[...])
            u_t = gate * (1.0 / (1.0 + jnp.exp(-gate))) * up
            u_buf[:, j * 256:(j + 1) * 256] = jnp.transpose(u_t).astype(BF16)
        ar_start(NB + b, u_buf[0:N], wdb)

    def own_resid(b, p):
        return gath[b, core, near, p]

    def final_rows(b):
        rows = ar_rows(NB + b)
        return normed(rows, gain(2))

    lane = lax.broadcasted_iota(jnp.int32, (1, TOK), 1)
    tgt_row = target[...] - shard * VOC

    M_OWN, S_OWN, TGT = 0, 1, 2
    kind = lax.broadcasted_iota(jnp.int32, (8, TOK), 0)
    blank = jnp.where(kind == M_OWN, NEG, 0.0)
    for e in range(NG + 1):
        stat[e] = blank

    def inside(e):
        first_tok, size, _ = GROUPS[e]
        return (lane >= first_tok) & (lane < first_tok + size)

    def turn(vals, e, j, back=False):
        shift = GROUPS[e][0] - j * GROUPS[e][1]
        shift = (-shift if back else shift) % TOK
        return pltpu.roll(vals, shift, 1) if shift else vals

    def packed_targets(e):
        wide = jnp.broadcast_to(tgt_row, (8, TOK))
        packed = turn(wide, e, 0, True)
        for j in range(1, GROUPS[e][2]):
            packed = jnp.where(lane >= j * GROUPS[e][1], turn(wide, e, j, True), packed)
        return packed[0:1]

    def own_update(z, b, rows, hit_row, lo, hi):
        live = (rows >= lo) & (rows < hi)
        zm = jnp.where(live, z, NEG)
        m_old = stat[b, M_OWN:M_OWN + 1]
        m_new = jnp.maximum(m_old, jnp.max(zm, axis=0, keepdims=True))
        s_add = jnp.sum(jnp.exp(zm - m_new), axis=0, keepdims=True)
        stat[b, S_OWN:S_OWN + 1] = stat[b, S_OWN:S_OWN + 1] * jnp.exp(m_old - m_new) + s_add
        stat[b, M_OWN:M_OWN + 1] = m_new
        hit = live & (rows == hit_row)
        stat[b, TGT:TGT + 1] = stat[b, TGT:TGT + 1] + jnp.sum(jnp.where(hit, z, 0.0), axis=0, keepdims=True)

    def packed_rows(e, i):
        rows = C // GROUPS[e][2]
        start = NCH * C * GROUPS[e][0] // TOK + i * rows
        return pl.ds(pl.multiple_of(start, 8), rows)

    def y_copy(e, i):
        where = packed_rows(e, i)
        arrived = y_r.at[e] if e < NG - 1 else y_r.at[e + i]
        return pltpu.make_async_remote_copy(
            src_ref=zsend.at[where], dst_ref=zrecv.at[where], send_sem=y_s.at[0], recv_sem=arrived,
            device_id=across, device_id_type=MESH)

    def next_load(g):
        @pl.when(g + NBUF < (NG + 1) * NCH)
        def _():
            w_load(g + NBUF).start()

    def send(e, start, stop):
        _, size, wide = GROUPS[e]
        rows = C // wide
        hit_row = packed_targets(e) - send_base
        packed_row = lax.broadcasted_iota(jnp.int32, (rows, TOK), 0) + lane // size * rows

        def send_chunk(i, carry):
            g = e * NCH + i
            w_load(g).wait()
            slot = g % NBUF
            acc = dot(wbuf[slot, 0:rows], hid_t[e])
            for j in range(1, wide):
                acc = jnp.where(lane >= j * size, dot(wbuf[slot, j * rows:(j + 1) * rows], hid_t[e]), acc)
            z = acc * INV_TEMP
            zsend[packed_rows(e, i)] = z
            y_copy(e, i).start()
            next_load(g)
            own_update(z, e, packed_row + i * C, hit_row, half * LAP, MID + half * LAP)
            return carry

        lax.fori_loop(start, stop, send_chunk, 0)

    keep_lo = (1 - half) * LAP
    keep_hi = MID + (1 - half) * LAP

    def keep():
        row_id = lax.broadcasted_iota(jnp.int32, (C, TOK), 0)
        hit_row = tgt_row - keep_base
        all_t = hid_t[0]
        for e in range(1, NG):
            all_t = jnp.where(lane >= GROUPS[e][0], hid_t[e], all_t)
        hid_all[...] = all_t

        def keep_chunk(i, carry):
            g = NG * NCH + i
            w_load(g).wait()
            z = dot(wbuf[g % NBUF], hid_all[...]) * INV_TEMP
            zkeep[i] = z
            next_load(g)
            own_update(z, NG, row_id + i * C, hit_row, keep_lo, keep_hi)
            return carry

        lax.fori_loop(0, NCH, keep_chunk, 0)

    def merge():
        for e in range(NG):
            for j in range(GROUPS[e][2]):
                moved = turn(stat[e], e, j)
                m_in, s_in = moved[M_OWN:M_OWN + 1], moved[S_OWN:S_OWN + 1]
                m_old = stat[NG, M_OWN:M_OWN + 1]
                s_old = stat[NG, S_OWN:S_OWN + 1]
                t_old = stat[NG, TGT:TGT + 1]
                m_new = jnp.maximum(m_old, m_in)
                s_new = s_old * jnp.exp(m_old - m_new) + s_in * jnp.exp(m_in - m_new)
                here = inside(e)
                stat[NG, M_OWN:M_OWN + 1] = jnp.where(here, m_new, m_old)
                stat[NG, S_OWN:S_OWN + 1] = jnp.where(here, s_new, s_old)
                stat[NG, TGT:TGT + 1] = jnp.where(here, t_old + moved[TGT:TGT + 1], t_old)

    def pair():
        row_q = lax.broadcasted_iota(jnp.int32, (QR, TOK), 0)

        def section(e, i, q):
            rows = C // GROUPS[e][2]
            start = NCH * C * GROUPS[e][0] // TOK + i * rows + q * QR % rows
            return turn(zrecv[pl.ds(pl.multiple_of(start, 8), QR)], e, q * QR // rows)

        def pair_chunk(i, carry):
            top, total = carry
            y_copy(NG - 1, i).wait_recv()
            for q in range(C // QR):
                rows = row_q + (i * C + q * QR)
                live = (rows >= keep_lo) & (rows < keep_hi)
                own = zkeep[i, q * QR:(q + 1) * QR]
                other = section(0, i, q)
                for e in range(1, NG):
                    other = jnp.where(lane >= GROUPS[e][0], section(e, i, q), other)
                z0 = jnp.where(pol, own, other)
                diff = jnp.where(pol, own - other, other - own)
                zm = jnp.where(live, z0, NEG)
                new_top = jnp.maximum(top, jnp.max(zm, axis=0, keepdims=True))
                total = total * jnp.exp(top - new_top) + jnp.sum(jnp.exp(zm - new_top) * diff, axis=0, keepdims=True)
                top = new_top
            return top, total

        for e in range(NG - 1):
            rows = NCH * C * GROUPS[e][1] // TOK
            all_of(zrecv.at[pl.ds(e * rows, rows)], y_s.at[0], y_r.at[e]).wait_recv()
        return lax.fori_loop(0, NCH, pair_chunk, (jnp.full((1, TOK), NEG, F32), jnp.zeros((1, TOK), F32)))

    def rows_out(b):
        hid_t[b] = jnp.transpose(jnp.concatenate([final_rows(b)] * (TOK // N), axis=0)).astype(BF16)

    steps = [
        ar_chip, lambda b: ar_own(b, functools.partial(own_x, b)), ar_relay, mlp,
        lambda b: ar_chip(NB + b), lambda b: ar_own(NB + b, functools.partial(own_resid, b)), lambda b: ar_relay(NB + b), rows_out,
    ]
    sent = [0] * NG
    for item in ",".join(ORDER).split(","):
        which = "abcd".find(item[0].lower())
        if which < 0:
            attend_rest()
        elif item[0].islower():
            steps[int(item[1:])](which)
        else:
            stop = sent[which] + int(item[1:])
            send(which, sent[which], stop)
            sent[which] = stop
    keep()
    for i in range(2 * NB):
        ar_drain(i)
    merge()

    def share_copy(n, k, slot):
        mine, theirs = ((own_shares, own_in), (cross_shares, cross_in))[n]
        return pltpu.make_async_remote_copy(
            src_ref=mine, dst_ref=theirs.at[slot], send_sem=f_s.at[n], recv_sem=f_r.at[n],
            device_id=rel_peer(k), device_id_type=MESH)

    def give(n):
        for k in range(1, 16):
            share_copy(n, k, me).start()

    def take(n):
        others = (own_in, cross_in)[n].at[pl.ds(0, 15)]
        all_of(others, f_s.at[n], f_r.at[n]).wait_recv()

    def normalizer(model):
        ids = [i for i in range(16) if (i % 4) // 2 == model]
        top = functools.reduce(jnp.maximum, [own_in[i, M_OWN:M_OWN + 1] for i in ids])
        tot = sum(own_in[i, S_OWN:S_OWN + 1] * jnp.exp(own_in[i, M_OWN:M_OWN + 1] - top) for i in ids)
        return top, tot

    own_shares[...] = stat[NG, 0:4]
    give(0)
    own_in[me] = stat[NG, 0:4]
    mine = jnp.concatenate(pair(), axis=0)
    cross_shares[...] = mine
    give(1)
    cross_in[me] = mine
    take(0)
    top0, tot0 = normalizer(0)
    top1, tot1 = normalizer(1)
    lse0, lse1 = top0 + jnp.log(tot0), top1 + jnp.log(tot1)
    tgt_z = sum(own_in[i, TGT:TGT + 1] for i in range(16) if (i % 4) // 2 == 0)
    take(1)
    cross = sum(cross_in[i, 1:2] * jnp.exp(cross_in[i, 0:1] - top0) for i in range(16))
    out[...] = jnp.concatenate([cross / tot0 - lse0 + lse1, tgt_z - lse0], axis=0)

    all_of(zsend, y_s.at[0], f_r.at[0]).wait_send()
    all_of(own_in.at[pl.ds(0, 15)], f_s.at[0], f_r.at[0]).wait_send()
    all_of(cross_in.at[pl.ds(0, 15)], f_s.at[1], f_r.at[1]).wait_send()


def solution(mesh):
    by_shard = P(("role", "tp"), None)
    by_role = P("role", None)

    def per_device(hidden, segment_ids, loss_mask, target, norm_gains, w_query, b_query, w_key, b_key, w_value, b_value, w_out, w_gate, w_up, w_down, w_head):
        anywhere = pl.BlockSpec(memory_space=pl.ANY)
        vmem = pl.BlockSpec(memory_space=pltpu.VMEM)
        dma = pltpu.SemaphoreType.DMA
        pair = pl.pallas_call(
            kernel,
            out_shape=jax.ShapeDtypeStruct((2, TOK), F32),
            in_specs=[anywhere] * 10 + [vmem] * 5,
            out_specs=vmem,
            scratch_shapes=[
                pltpu.VMEM((TOK, D), BF16),
                pltpu.VMEM((3, 2, D), F32),
                pltpu.VMEM((384, D), BF16),
                pltpu.VMEM((256, D), BF16),
                pltpu.VMEM((FF, D), BF16),
                pltpu.VMEM((FF, D), BF16),
                pltpu.VMEM((FF, D), BF16),
                pltpu.VMEM((NBUF, C, D), BF16),
                pltpu.VMEM((TOK, TOK), F32),
                pltpu.VMEM((D, TOK), BF16),
                pltpu.VMEM((2 * NB, 2, N, DH), F32),
                pltpu.VMEM((2 * NB, N, DH), F32),
                pltpu.VMEM((2 * NB, 2, 2, PR, DH), F32),
                pltpu.VMEM((2 * NB, 2, 3, PR, DH), F32),
                pltpu.VMEM((2 * NB, 2, 2, 2, PR, DH), F32),
                pltpu.VMEM((NG, D, TOK), BF16),
                pltpu.VMEM((D, TOK), BF16),
                pltpu.VMEM((TOK, FF), BF16),
                pltpu.VMEM((BLK, TOK), F32),
                pltpu.VMEM((BLK, TOK), F32),
                pltpu.VMEM((NCH, C, TOK), F32),
                pltpu.VMEM((NG + 1, 8, TOK), F32),
                pltpu.VMEM((4, TOK), F32),
                pltpu.VMEM((16, 4, TOK), F32),
                pltpu.VMEM((2, TOK), F32),
                pltpu.VMEM((16, 2, TOK), F32),
                dma((9,)), dma((NBUF,)),
                dma((2 * NB,)), dma((2 * NB,)), dma((2 * NB, 2)), dma((2 * NB, 4)), dma((2 * NB,)),
                dma((1,)), dma((NG - 1 + NCH,)), dma((2,)), dma((2,)),
            ],
            compiler_params=pltpu.CompilerParams(
                collective_id=0, has_side_effects=True, vmem_limit_bytes=60 * 1024 * 1024),
        )(hidden, w_query, w_key, w_value, w_out, w_gate, w_up, w_down, w_head, jnp.swapaxes(norm_gains, 0, 1),
          segment_ids.reshape(1, TOK), target.reshape(1, TOK), b_query, b_key, b_value)
        found = loss_mask.astype(F32)
        return pair[0] * found, pair[1] * found

    in_specs = (P(None, "dp", None), P("dp"), P("dp"), P("dp"), P(None, None, None), by_shard, by_shard, by_role, by_role, by_role, by_role, by_shard, by_shard, by_shard, by_shard, by_shard)
    return jax.shard_map(per_device, mesh=mesh, in_specs=in_specs, out_specs=(P("dp"), P("dp")), check_vma=False)
```

```python
import functools
import math

import jax
import jax.numpy as jnp
from jax import lax
from jax.experimental import pallas as pl
from jax.experimental.pallas import tpu as pltpu
from jax.sharding import PartitionSpec as P

MESH = pl.DeviceIdType.MESH
F32 = jnp.float32
BF16 = jnp.bfloat16
EPS = 1e-6
LOG_BASE = math.log(1000000.0)
INV_TEMP = 1.0 / 0.7

TOK = 128
D = 2048
DH = D // 2
HEAD = 64
QH = 4
FF = 1024
VOC = 16032
MID = VOC // 2
C = 576
NCH = 14
BLK = C * NCH
OFF = VOC - BLK
LAP = BLK - MID
NBUF = 4
NB = 4
N = TOK // NB
GROUPS = ((0, 32, 4), (32, 32, 4), (64, 32, 4), (96, 32, 4))
NG = len(GROUPS)
QR = C // 4
NZ = 4
NH = N // 2
PR = NH // 2
NEG = -1e30
ORDER = (
    "a0,x,a1,a2,b0,a3,a4,a5,a6,b1,a7",
    "A2,c0,A1,b2,A2,b3,A1,b4,c1,A6,b5,A2,c2,b6,d0,b7",
    "B2,c3,d1,B2,c4,B4,d2,B2,c5,d3,B2,d4,c6,B2,c7",
    "C4,d5,C4,d6,C2,d7,C4,D14",
)


def dot(lhs, rhs):
    return jnp.dot(lhs, rhs, preferred_element_type=F32)


def kernel(hid, wq, wk, wv, wo, wg, wu, wd, wh, gains, seg, target, bq, bk, bv,
           out,
           xb, gain_in, wqkv, wob, wgb, wub, wdb, wbuf, tr, act_t, part, core_in, chip_sum, rs_in, gath, hid_t, hid_all,
           u_buf, zsend, zrecv, zkeep, stat, own_shares, own_in, cross_shares, cross_in,
           in_sem, w_sem, ar_s, d_r, rs_r, ag_r, rl_r, y_s, y_r, f_s, f_r):
    dp, tp, ro = lax.axis_index("dp"), lax.axis_index("tp"), lax.axis_index("role")
    half, core = ro // 2, ro % 2
    shard = core * NZ + tp
    me = tp * 4 + ro
    pol = half == 0
    partner = (dp, tp, ro + 1 - 2 * core)
    across = (dp, tp, (ro + 2) % 4)

    def z_peer(k):
        return (dp, (tp + k) % NZ, ro)

    def rel_peer(k):
        other = (me + k) % 16
        return (dp, other // 4, other % 4)

    loads = [
        pltpu.make_async_copy(hid.at[half], xb, in_sem.at[0]),
        pltpu.make_async_copy(wq, wqkv.at[pl.ds(0, 256)], in_sem.at[1]),
        pltpu.make_async_copy(wk.at[pl.ds(pl.multiple_of(tp * HEAD, HEAD), HEAD)], wqkv.at[pl.ds(256, HEAD)], in_sem.at[2]),
        pltpu.make_async_copy(wv.at[pl.ds(pl.multiple_of(tp * HEAD, HEAD), HEAD)], wqkv.at[pl.ds(320, HEAD)], in_sem.at[3]),
        pltpu.make_async_copy(wo, wob, in_sem.at[4]),
        pltpu.make_async_copy(wg, wgb, in_sem.at[5]),
        pltpu.make_async_copy(wu, wub, in_sem.at[6]),
        pltpu.make_async_copy(wd, wdb, in_sem.at[7]),
        pltpu.make_async_copy(gains, gain_in, in_sem.at[8]),
    ]
    first_loads = loads[0:4] + loads[8:9]
    for copy in first_loads:
        copy.start()

    barrier = pltpu.get_barrier_semaphore()
    for k in range(1, 16):
        pl.semaphore_signal(barrier, inc=1, device_id=rel_peer(k), device_id_type=MESH)

    send_base = half * OFF
    keep_base = (1 - half) * OFF

    def w_load(g):
        kept = g // NCH >= NG
        base = jnp.where(kept, keep_base, send_base) + (g % NCH) * C
        slot = g % NBUF
        return pltpu.make_async_copy(wh.at[pl.ds(pl.multiple_of(base, 16), C)], wbuf.at[slot], w_sem.at[slot])

    rows8 = lax.broadcasted_iota(jnp.int32, (QH, HEAD), 0)
    tr[...] = jnp.zeros_like(tr)
    tr[0:QH, 0:HEAD] = bq[...].astype(F32)
    pick = rows8 == tp
    tr[QH:QH + 1, 0:HEAD] = jnp.sum(jnp.where(pick, bk[...].astype(F32), 0.0), axis=0, keepdims=True)
    tr[QH + 1:QH + 2, 0:HEAD] = jnp.sum(jnp.where(pick, bv[...].astype(F32), 0.0), axis=0, keepdims=True)
    seg_row = seg[...].astype(F32)
    tr[QH + 2:QH + 3, :] = seg_row
    cols = jnp.transpose(tr[...])
    seg_col = cols[:, QH + 2:QH + 3]
    src_id = lax.broadcasted_iota(jnp.int32, (TOK, TOK), 0)
    dst_id = lax.broadcasted_iota(jnp.int32, (TOK, TOK), 1)
    allowed = (seg_col == seg_row) & (src_id <= dst_id)
    pos = jnp.sum(jnp.where(allowed, 1.0, 0.0), axis=0, keepdims=True) - 1.0
    rot_id = lax.broadcasted_iota(jnp.int32, (HEAD // 2, TOK), 0).astype(F32)
    angles = pos * jnp.exp(rot_id * (-2.0 * LOG_BASE / HEAD))
    cos_part, sin_part = jnp.cos(angles), jnp.sin(angles)

    def normed(rows, scale):
        inv = lax.rsqrt(jnp.mean(rows * rows, axis=-1, keepdims=True) + EPS)
        return rows * inv * scale

    loads[0].wait()
    loads[8].wait()

    def gain(k):
        return jnp.where(pol, gain_in[k, 0:1], gain_in[k, 1:2])

    def rotate(vals, n):
        lo, hi = vals[:HEAD // 2], vals[HEAD // 2:]
        cos_n, sin_n = cos_part[:, :n], sin_part[:, :n]
        return jnp.concatenate([lo * cos_n - hi * sin_n, hi * cos_n + lo * sin_n], axis=0)

    def attention(n):
        rows_t = jnp.transpose(normed(xb[0:n].astype(F32), gain(0))).astype(BF16)
        qkv = dot(wqkv[...], rows_t)
        key = jnp.transpose(rotate(qkv[256:320] + cols[0:HEAD, QH:QH + 1], n)).astype(BF16)
        val_t = (qkv[320:384] + cols[0:HEAD, QH + 1:QH + 2]).astype(BF16)
        outs = []
        for h in range(QH):
            query = rotate(qkv[h * HEAD:(h + 1) * HEAD] + cols[0:HEAD, h:h + 1], n).astype(BF16)
            scores = jnp.where(allowed[0:n, 0:n], dot(key, query) * (HEAD ** -0.5), NEG)
            weights = jnp.exp(scores - jnp.max(scores, axis=0, keepdims=True))
            probs = (weights / jnp.sum(weights, axis=0, keepdims=True)).astype(BF16)
            outs.append(dot(val_t, probs))
        return jnp.transpose(jnp.concatenate(outs, axis=0)).astype(BF16)

    for copy in loads[1:4]:
        copy.wait()
    for copy in loads[4:8]:
        copy.start()
    for g in range(NBUF):
        w_load(g).start()
    attn = attention(N)
    loads[4].wait()
    pl.semaphore_wait(barrier, 15)

    mid = (tp == 1) | (tp == 2)
    near = tp // 2
    far = 1 - near

    def copies_core(i):
        return pltpu.make_async_remote_copy(
            src_ref=part.at[i, 1 - core], dst_ref=core_in.at[i], send_sem=ar_s.at[i], recv_sem=d_r.at[i],
            device_id=partner, device_id_type=MESH)

    def copies_rs(i, o, slot, p):
        return pltpu.make_async_remote_copy(
            src_ref=chip_sum.at[i, o, p], dst_ref=rs_in.at[i, p, slot], send_sem=ar_s.at[i],
            recv_sem=rs_r.at[i, p], device_id=(dp, 1 + o, ro), device_id_type=MESH)

    def copies_ag(i, o, k, p):
        return pltpu.make_async_remote_copy(
            src_ref=gath.at[i, core, o, p], dst_ref=gath.at[i, core, o, p], send_sem=ar_s.at[i],
            recv_sem=ag_r.at[i, 2 * o + p], device_id=z_peer(k), device_id_type=MESH)

    def copies_relay(i, side, o, p):
        return pltpu.make_async_remote_copy(
            src_ref=gath.at[i, side, o, p], dst_ref=gath.at[i, side, o, p],
            send_sem=ar_s.at[i], recv_sem=rl_r.at[i], device_id=partner, device_id_type=MESH)

    def all_of(ref, send_sem, recv_sem):
        return pltpu.make_async_remote_copy(
            src_ref=ref, dst_ref=ref, send_sem=send_sem, recv_sem=recv_sem, device_id=partner, device_id_type=MESH)

    def ar_start(i, lhs, w_ref):
        theirs = pl.ds(pl.multiple_of((1 - core) * DH, DH), DH)
        ours = pl.ds(pl.multiple_of(core * DH, DH), DH)
        part[i, 1 - core] = dot(lhs, w_ref[:, theirs])
        copies_core(i).start()
        part[i, core] = dot(lhs, w_ref[:, ours])

    def ar_chip(i):
        copies_core(i).wait_recv()
        chip_sum[i] = (part[i, core] + core_in[i]).reshape(2, 2, PR, DH)
        for p in range(2):
            copies_rs(i, far, jnp.where(tp < 1 + far, tp, tp - 1), p).start()

            @pl.when(jnp.logical_not(mid))
            def _():
                copies_rs(i, near, jnp.where(tp < 1 + near, tp, tp - 1), p).start()

    def ar_own(i, before):
        @pl.when(mid)
        def _():
            for p in range(2):
                all_of(rs_in.at[i, p], ar_s.at[i], rs_r.at[i, p]).wait_recv()
                total = chip_sum[i, near, p] + rs_in[i, p, 0] + rs_in[i, p, 1] + rs_in[i, p, 2]
                gath[i, core, near, p] = (before(p) + total).astype(BF16).astype(F32)
                for k in (2, 1, 3):
                    copies_ag(i, near, k, p).start()
                copies_relay(i, core, near, p).start()

    def ar_relay(i):
        for p in range(2):
            @pl.when(jnp.logical_not(mid))
            def _():
                copies_ag(i, near, 1, p).wait_recv()
                copies_relay(i, core, near, p).start()

            copies_ag(i, far, 1, p).wait_recv()
            copies_relay(i, core, far, p).start()

    def ar_rows(i):
        all_of(gath.at[i, 1 - core], ar_s.at[i], rl_r.at[i]).wait_recv()
        return jnp.concatenate([gath[i, 0].reshape(N, DH), gath[i, 1].reshape(N, DH)], axis=1)

    def ar_drain(i):
        @pl.when(mid)
        def _():
            all_of(gath.at[pl.ds(0, 2)], ar_s.at[i], rl_r.at[i]).wait_send()

        @pl.when(jnp.logical_not(mid))
        def _():
            all_of(rs_in.at[pl.ds(0, 2)], ar_s.at[i], rl_r.at[i]).wait_send()

    ar_start(0, attn, wob)

    def attend_rest():
        heads = attention(TOK)
        for b in range(1, NB):
            ar_start(b, heads[b * N:(b + 1) * N], wob)

    def own_x(b, p):
        rows = pl.ds(pl.multiple_of(b * N + near * NH + p * PR, 8), PR)
        return jnp.where(core == 0, xb[rows, 0:DH].astype(F32), xb[rows, DH:D].astype(F32))

    def mlp(b):
        rows = ar_rows(b)
        b_t = jnp.transpose(jnp.concatenate([normed(rows, gain(1))] * (TOK // N), axis=0)).astype(BF16)
        act_t[...] = b_t
        if b == 0:
            for copy in loads[5:8]:
                copy.wait()
        for j in range(4):
            gate = dot(wgb[j * 256:(j + 1) * 256], act_t[...])
            up = dot(wub[j * 256:(j + 1) * 256], act_t[...])
            u_t = gate * (1.0 / (1.0 + jnp.exp(-gate))) * up
            u_buf[:, j * 256:(j + 1) * 256] = jnp.transpose(u_t).astype(BF16)
        ar_start(NB + b, u_buf[0:N], wdb)

    def own_resid(b, p):
        return gath[b, core, near, p]

    def final_rows(b):
        rows = ar_rows(NB + b)
        return normed(rows, gain(2))

    lane = lax.broadcasted_iota(jnp.int32, (1, TOK), 1)
    tgt_row = target[...] - shard * VOC

    M_OWN, S_OWN, TGT = 0, 1, 2
    kind = lax.broadcasted_iota(jnp.int32, (8, TOK), 0)
    blank = jnp.where(kind == M_OWN, NEG, 0.0)
    for e in range(NG + 1):
        stat[e] = blank

    def inside(e):
        first_tok, size, _ = GROUPS[e]
        return (lane >= first_tok) & (lane < first_tok + size)

    def turn(vals, e, j, back=False):
        shift = GROUPS[e][0] - j * GROUPS[e][1]
        shift = (-shift if back else shift) % TOK
        return pltpu.roll(vals, shift, 1) if shift else vals

    def packed_targets(e):
        wide = jnp.broadcast_to(tgt_row, (8, TOK))
        packed = turn(wide, e, 0, True)
        for j in range(1, GROUPS[e][2]):
            packed = jnp.where(lane >= j * GROUPS[e][1], turn(wide, e, j, True), packed)
        return packed[0:1]

    def own_update(z, b, rows, hit_row, lo, hi):
        live = (rows >= lo) & (rows < hi)
        zm = jnp.where(live, z, NEG)
        m_old = stat[b, M_OWN:M_OWN + 1]
        m_new = jnp.maximum(m_old, jnp.max(zm, axis=0, keepdims=True))
        s_add = jnp.sum(jnp.exp(zm - m_new), axis=0, keepdims=True)
        stat[b, S_OWN:S_OWN + 1] = stat[b, S_OWN:S_OWN + 1] * jnp.exp(m_old - m_new) + s_add
        stat[b, M_OWN:M_OWN + 1] = m_new
        hit = live & (rows == hit_row)
        stat[b, TGT:TGT + 1] = stat[b, TGT:TGT + 1] + jnp.sum(jnp.where(hit, z, 0.0), axis=0, keepdims=True)

    def packed_rows(e, i):
        rows = C // GROUPS[e][2]
        start = NCH * C * GROUPS[e][0] // TOK + i * rows
        return pl.ds(pl.multiple_of(start, 8), rows)

    def y_copy(e, i):
        where = packed_rows(e, i)
        arrived = y_r.at[e] if e < NG - 1 else y_r.at[e + i]
        return pltpu.make_async_remote_copy(
            src_ref=zsend.at[where], dst_ref=zrecv.at[where], send_sem=y_s.at[0], recv_sem=arrived,
            device_id=across, device_id_type=MESH)

    def next_load(g):
        @pl.when(g + NBUF < (NG + 1) * NCH)
        def _():
            w_load(g + NBUF).start()

    def send(e, start, stop):
        _, size, wide = GROUPS[e]
        rows = C // wide
        hit_row = packed_targets(e) - send_base
        packed_row = lax.broadcasted_iota(jnp.int32, (rows, TOK), 0) + lane // size * rows

        def send_chunk(i, carry):
            g = e * NCH + i
            w_load(g).wait()
            slot = g % NBUF
            acc = dot(wbuf[slot, 0:rows], hid_t[e])
            for j in range(1, wide):
                acc = jnp.where(lane >= j * size, dot(wbuf[slot, j * rows:(j + 1) * rows], hid_t[e]), acc)
            z = acc * INV_TEMP
            zsend[packed_rows(e, i)] = z
            y_copy(e, i).start()
            next_load(g)
            own_update(z, e, packed_row + i * C, hit_row, half * LAP, MID + half * LAP)
            return carry

        lax.fori_loop(start, stop, send_chunk, 0)

    keep_lo = (1 - half) * LAP
    keep_hi = MID + (1 - half) * LAP

    def keep():
        row_id = lax.broadcasted_iota(jnp.int32, (C, TOK), 0)
        hit_row = tgt_row - keep_base
        all_t = hid_t[0]
        for e in range(1, NG):
            all_t = jnp.where(lane >= GROUPS[e][0], hid_t[e], all_t)
        hid_all[...] = all_t

        def keep_chunk(i, carry):
            g = NG * NCH + i
            w_load(g).wait()
            z = dot(wbuf[g % NBUF], hid_all[...]) * INV_TEMP
            zkeep[i] = z
            next_load(g)
            own_update(z, NG, row_id + i * C, hit_row, keep_lo, keep_hi)
            return carry

        lax.fori_loop(0, NCH, keep_chunk, 0)

    def merge():
        for e in range(NG):
            for j in range(GROUPS[e][2]):
                moved = turn(stat[e], e, j)
                m_in, s_in = moved[M_OWN:M_OWN + 1], moved[S_OWN:S_OWN + 1]
                m_old = stat[NG, M_OWN:M_OWN + 1]
                s_old = stat[NG, S_OWN:S_OWN + 1]
                t_old = stat[NG, TGT:TGT + 1]
                m_new = jnp.maximum(m_old, m_in)
                s_new = s_old * jnp.exp(m_old - m_new) + s_in * jnp.exp(m_in - m_new)
                here = inside(e)
                stat[NG, M_OWN:M_OWN + 1] = jnp.where(here, m_new, m_old)
                stat[NG, S_OWN:S_OWN + 1] = jnp.where(here, s_new, s_old)
                stat[NG, TGT:TGT + 1] = jnp.where(here, t_old + moved[TGT:TGT + 1], t_old)

    def pair():
        row_q = lax.broadcasted_iota(jnp.int32, (QR, TOK), 0)

        def section(e, i, q):
            rows = C // GROUPS[e][2]
            start = NCH * C * GROUPS[e][0] // TOK + i * rows + q * QR % rows
            return turn(zrecv[pl.ds(pl.multiple_of(start, 8), QR)], e, q * QR // rows)

        def pair_chunk(i, carry):
            top, total = carry
            y_copy(NG - 1, i).wait_recv()
            for q in range(C // QR):
                rows = row_q + (i * C + q * QR)
                live = (rows >= keep_lo) & (rows < keep_hi)
                own = zkeep[i, q * QR:(q + 1) * QR]
                other = section(0, i, q)
                for e in range(1, NG):
                    other = jnp.where(lane >= GROUPS[e][0], section(e, i, q), other)
                z0 = jnp.where(pol, own, other)
                diff = jnp.where(pol, own - other, other - own)
                zm = jnp.where(live, z0, NEG)
                new_top = jnp.maximum(top, jnp.max(zm, axis=0, keepdims=True))
                total = total * jnp.exp(top - new_top) + jnp.sum(jnp.exp(zm - new_top) * diff, axis=0, keepdims=True)
                top = new_top
            return top, total

        for e in range(NG - 1):
            rows = NCH * C * GROUPS[e][1] // TOK
            all_of(zrecv.at[pl.ds(e * rows, rows)], y_s.at[0], y_r.at[e]).wait_recv()
        return lax.fori_loop(0, NCH, pair_chunk, (jnp.full((1, TOK), NEG, F32), jnp.zeros((1, TOK), F32)))

    def rows_out(b):
        hid_t[b] = jnp.transpose(jnp.concatenate([final_rows(b)] * (TOK // N), axis=0)).astype(BF16)

    steps = [
        ar_chip, lambda b: ar_own(b, functools.partial(own_x, b)), ar_relay, mlp,
        lambda b: ar_chip(NB + b), lambda b: ar_own(NB + b, functools.partial(own_resid, b)), lambda b: ar_relay(NB + b), rows_out,
    ]
    sent = [0] * NG
    for item in ",".join(ORDER).split(","):
        which = "abcd".find(item[0].lower())
        if which < 0:
            attend_rest()
        elif item[0].islower():
            steps[int(item[1:])](which)
        else:
            stop = sent[which] + int(item[1:])
            send(which, sent[which], stop)
            sent[which] = stop
    keep()
    for i in range(2 * NB):
        ar_drain(i)
    merge()

    def share_copy(n, k, slot):
        mine, theirs = ((own_shares, own_in), (cross_shares, cross_in))[n]
        return pltpu.make_async_remote_copy(
            src_ref=mine, dst_ref=theirs.at[slot], send_sem=f_s.at[n], recv_sem=f_r.at[n],
            device_id=rel_peer(k), device_id_type=MESH)

    def give(n):
        for k in range(1, 16):
            share_copy(n, k, me).start()

    def take(n):
        others = (own_in, cross_in)[n].at[pl.ds(0, 15)]
        all_of(others, f_s.at[n], f_r.at[n]).wait_recv()

    def normalizer(model):
        ids = [i for i in range(16) if (i % 4) // 2 == model]
        top = functools.reduce(jnp.maximum, [own_in[i, M_OWN:M_OWN + 1] for i in ids])
        tot = sum(own_in[i, S_OWN:S_OWN + 1] * jnp.exp(own_in[i, M_OWN:M_OWN + 1] - top) for i in ids)
        return top, tot

    own_shares[...] = stat[NG, 0:4]
    give(0)
    own_in[me] = stat[NG, 0:4]
    mine = jnp.concatenate(pair(), axis=0)
    cross_shares[...] = mine
    give(1)
    cross_in[me] = mine
    take(0)
    top0, tot0 = normalizer(0)
    top1, tot1 = normalizer(1)
    lse0, lse1 = top0 + jnp.log(tot0), top1 + jnp.log(tot1)
    tgt_z = sum(own_in[i, TGT:TGT + 1] for i in range(16) if (i % 4) // 2 == 0)
    take(1)
    cross = sum(cross_in[i, 1:2] * jnp.exp(cross_in[i, 0:1] - top0) for i in range(16))
    out[...] = jnp.concatenate([cross / tot0 - lse0 + lse1, tgt_z - lse0], axis=0)

    all_of(zsend, y_s.at[0], f_r.at[0]).wait_send()
    all_of(own_in.at[pl.ds(0, 15)], f_s.at[0], f_r.at[0]).wait_send()
    all_of(cross_in.at[pl.ds(0, 15)], f_s.at[1], f_r.at[1]).wait_send()


def solution(mesh):
    by_shard = P(("role", "tp"), None)
    by_role = P("role", None)

    def per_device(hidden, segment_ids, loss_mask, target, norm_gains, w_query, b_query, w_key, b_key, w_value, b_value, w_out, w_gate, w_up, w_down, w_head):
        anywhere = pl.BlockSpec(memory_space=pl.ANY)
        vmem = pl.BlockSpec(memory_space=pltpu.VMEM)
        dma = pltpu.SemaphoreType.DMA
        pair = pl.pallas_call(
            kernel,
            out_shape=jax.ShapeDtypeStruct((2, TOK), F32),
            in_specs=[anywhere] * 10 + [vmem] * 5,
            out_specs=vmem,
            scratch_shapes=[
                pltpu.VMEM((TOK, D), BF16),
                pltpu.VMEM((3, 2, D), F32),
                pltpu.VMEM((384, D), BF16),
                pltpu.VMEM((256, D), BF16),
                pltpu.VMEM((FF, D), BF16),
                pltpu.VMEM((FF, D), BF16),
                pltpu.VMEM((FF, D), BF16),
                pltpu.VMEM((NBUF, C, D), BF16),
                pltpu.VMEM((TOK, TOK), F32),
                pltpu.VMEM((D, TOK), BF16),
                pltpu.VMEM((2 * NB, 2, N, DH), F32),
                pltpu.VMEM((2 * NB, N, DH), F32),
                pltpu.VMEM((2 * NB, 2, 2, PR, DH), F32),
                pltpu.VMEM((2 * NB, 2, 3, PR, DH), F32),
                pltpu.VMEM((2 * NB, 2, 2, 2, PR, DH), F32),
                pltpu.VMEM((NG, D, TOK), BF16),
                pltpu.VMEM((D, TOK), BF16),
                pltpu.VMEM((TOK, FF), BF16),
                pltpu.VMEM((BLK, TOK), F32),
                pltpu.VMEM((BLK, TOK), F32),
                pltpu.VMEM((NCH, C, TOK), F32),
                pltpu.VMEM((NG + 1, 8, TOK), F32),
                pltpu.VMEM((4, TOK), F32),
                pltpu.VMEM((16, 4, TOK), F32),
                pltpu.VMEM((2, TOK), F32),
                pltpu.VMEM((16, 2, TOK), F32),
                dma((9,)), dma((NBUF,)),
                dma((2 * NB,)), dma((2 * NB,)), dma((2 * NB, 2)), dma((2 * NB, 4)), dma((2 * NB,)),
                dma((1,)), dma((NG - 1 + NCH,)), dma((2,)), dma((2,)),
            ],
            compiler_params=pltpu.CompilerParams(
                collective_id=0, has_side_effects=True, vmem_limit_bytes=60 * 1024 * 1024),
        )(hidden, w_query, w_key, w_value, w_out, w_gate, w_up, w_down, w_head, jnp.swapaxes(norm_gains, 0, 1),
          segment_ids.reshape(1, TOK), target.reshape(1, TOK), b_query, b_key, b_value)
        found = loss_mask.astype(F32)
        return pair[0] * found, pair[1] * found

    in_specs = (P(None, "dp", None), P("dp"), P("dp"), P("dp"), P(None, None, None), by_shard, by_shard, by_role, by_role, by_role, by_role, by_shard, by_shard, by_shard, by_shard, by_shard)
    return jax.shard_map(per_device, mesh=mesh, in_specs=in_specs, out_specs=(P("dp"), P("dp")), check_vma=False)
```

```python
import functools
import math

import jax
import jax.numpy as jnp
from jax import lax
from jax.experimental import pallas as pl
from jax.experimental.pallas import tpu as pltpu
from jax.sharding import PartitionSpec as P

MESH = pl.DeviceIdType.MESH
F32 = jnp.float32
BF16 = jnp.bfloat16
EPS = 1e-6
LOG_BASE = math.log(1000000.0)
INV_TEMP = 1.0 / 0.7

TOK = 128
D = 2048
DH = D // 2
HEAD = 64
QH = 4
FF = 1024
VOC = 16032
MID = VOC // 2
C = 576
NCH = 14
BLK = C * NCH
OFF = VOC - BLK
LAP = BLK - MID
NBUF = 4
NB = 4
N = TOK // NB
GROUPS = ((0, 32, 4), (32, 32, 4), (64, 32, 4), (96, 32, 4))
NG = len(GROUPS)
QR = C // 4
NZ = 4
NH = N // 2
PR = NH // 2
NEG = -1e30
ORDER = (
    "a0,x,a1,a2,b0,a3,a4,a5,a6,b1,a7",
    "A2,c0,A1,b2,A2,b3,A1,b4,c1,A6,b5,A2,c2,b6,d0,b7",
    "B2,c3,d1,B2,c4,B4,d2,B2,c5,d3,B2,d4,c6,B2,c7",
    "C4,d5,C4,d6,C2,d7,C4,D14",
)


def dot(lhs, rhs):
    return jnp.dot(lhs, rhs, preferred_element_type=F32)


def kernel(hid, wq, wk, wv, wo, wg, wu, wd, wh, gains, seg, target, bq, bk, bv,
           out,
           xb, gain_in, wqkv, wob, wgb, wub, wdb, wbuf, tr, act_t, part, core_in, chip_sum, rs_in, gath, hid_t, hid_all,
           u_buf, zsend, zrecv, zkeep, stat, own_shares, own_in, cross_shares, cross_in,
           in_sem, w_sem, ar_s, d_r, rs_r, ag_r, rl_r, y_s, y_r, f_s, f_r):
    dp, tp, ro = lax.axis_index("dp"), lax.axis_index("tp"), lax.axis_index("role")
    half, core = ro // 2, ro % 2
    shard = core * NZ + tp
    me = tp * 4 + ro
    pol = half == 0
    partner = (dp, tp, ro + 1 - 2 * core)
    across = (dp, tp, (ro + 2) % 4)

    def z_peer(k):
        return (dp, (tp + k) % NZ, ro)

    def rel_peer(k):
        other = (me + k) % 16
        return (dp, other // 4, other % 4)

    loads = [
        pltpu.make_async_copy(hid.at[half], xb, in_sem.at[0]),
        pltpu.make_async_copy(wq, wqkv.at[pl.ds(0, 256)], in_sem.at[1]),
        pltpu.make_async_copy(wk.at[pl.ds(pl.multiple_of(tp * HEAD, HEAD), HEAD)], wqkv.at[pl.ds(256, HEAD)], in_sem.at[2]),
        pltpu.make_async_copy(wv.at[pl.ds(pl.multiple_of(tp * HEAD, HEAD), HEAD)], wqkv.at[pl.ds(320, HEAD)], in_sem.at[3]),
        pltpu.make_async_copy(wo, wob, in_sem.at[4]),
        pltpu.make_async_copy(wg, wgb, in_sem.at[5]),
        pltpu.make_async_copy(wu, wub, in_sem.at[6]),
        pltpu.make_async_copy(wd, wdb, in_sem.at[7]),
        pltpu.make_async_copy(gains, gain_in, in_sem.at[8]),
    ]
    first_loads = loads[0:4] + loads[8:9]
    for copy in first_loads:
        copy.start()

    barrier = pltpu.get_barrier_semaphore()
    for k in range(1, 16):
        pl.semaphore_signal(barrier, inc=1, device_id=rel_peer(k), device_id_type=MESH)

    send_base = half * OFF
    keep_base = (1 - half) * OFF

    def w_load(g):
        kept = g // NCH >= NG
        base = jnp.where(kept, keep_base, send_base) + (g % NCH) * C
        slot = g % NBUF
        return pltpu.make_async_copy(wh.at[pl.ds(pl.multiple_of(base, 16), C)], wbuf.at[slot], w_sem.at[slot])

    rows8 = lax.broadcasted_iota(jnp.int32, (QH, HEAD), 0)
    tr[...] = jnp.zeros_like(tr)
    tr[0:QH, 0:HEAD] = bq[...].astype(F32)
    pick = rows8 == tp
    tr[QH:QH + 1, 0:HEAD] = jnp.sum(jnp.where(pick, bk[...].astype(F32), 0.0), axis=0, keepdims=True)
    tr[QH + 1:QH + 2, 0:HEAD] = jnp.sum(jnp.where(pick, bv[...].astype(F32), 0.0), axis=0, keepdims=True)
    seg_row = seg[...].astype(F32)
    tr[QH + 2:QH + 3, :] = seg_row
    cols = jnp.transpose(tr[...])
    seg_col = cols[:, QH + 2:QH + 3]
    src_id = lax.broadcasted_iota(jnp.int32, (TOK, TOK), 0)
    dst_id = lax.broadcasted_iota(jnp.int32, (TOK, TOK), 1)
    allowed = (seg_col == seg_row) & (src_id <= dst_id)
    pos = jnp.sum(jnp.where(allowed, 1.0, 0.0), axis=0, keepdims=True) - 1.0
    rot_id = lax.broadcasted_iota(jnp.int32, (HEAD // 2, TOK), 0).astype(F32)
    angles = pos * jnp.exp(rot_id * (-2.0 * LOG_BASE / HEAD))
    cos_part, sin_part = jnp.cos(angles), jnp.sin(angles)

    def normed(rows, scale):
        inv = lax.rsqrt(jnp.mean(rows * rows, axis=-1, keepdims=True) + EPS)
        return rows * inv * scale

    loads[0].wait()
    loads[8].wait()

    def gain(k):
        return jnp.where(pol, gain_in[k, 0:1], gain_in[k, 1:2])

    def rotate(vals, n):
        lo, hi = vals[:HEAD // 2], vals[HEAD // 2:]
        cos_n, sin_n = cos_part[:, :n], sin_part[:, :n]
        return jnp.concatenate([lo * cos_n - hi * sin_n, hi * cos_n + lo * sin_n], axis=0)

    def attention(n):
        rows_t = jnp.transpose(normed(xb[0:n].astype(F32), gain(0))).astype(BF16)
        qkv = dot(wqkv[...], rows_t)
        key = jnp.transpose(rotate(qkv[256:320] + cols[0:HEAD, QH:QH + 1], n)).astype(BF16)
        val_t = (qkv[320:384] + cols[0:HEAD, QH + 1:QH + 2]).astype(BF16)
        outs = []
        for h in range(QH):
            query = rotate(qkv[h * HEAD:(h + 1) * HEAD] + cols[0:HEAD, h:h + 1], n).astype(BF16)
            scores = jnp.where(allowed[0:n, 0:n], dot(key, query) * (HEAD ** -0.5), NEG)
            weights = jnp.exp(scores - jnp.max(scores, axis=0, keepdims=True))
            probs = (weights / jnp.sum(weights, axis=0, keepdims=True)).astype(BF16)
            outs.append(dot(val_t, probs))
        return jnp.transpose(jnp.concatenate(outs, axis=0)).astype(BF16)

    for copy in loads[1:4]:
        copy.wait()
    for copy in loads[4:8]:
        copy.start()
    for g in range(NBUF):
        w_load(g).start()
    attn = attention(N)
    loads[4].wait()
    pl.semaphore_wait(barrier, 15)

    mid = (tp == 1) | (tp == 2)
    near = tp // 2
    far = 1 - near

    def copies_core(i):
        return pltpu.make_async_remote_copy(
            src_ref=part.at[i, 1 - core], dst_ref=core_in.at[i], send_sem=ar_s.at[i], recv_sem=d_r.at[i],
            device_id=partner, device_id_type=MESH)

    def copies_rs(i, o, slot, p):
        return pltpu.make_async_remote_copy(
            src_ref=chip_sum.at[i, o, p], dst_ref=rs_in.at[i, p, slot], send_sem=ar_s.at[i],
            recv_sem=rs_r.at[i, p], device_id=(dp, 1 + o, ro), device_id_type=MESH)

    def copies_ag(i, o, k, p):
        return pltpu.make_async_remote_copy(
            src_ref=gath.at[i, core, o, p], dst_ref=gath.at[i, core, o, p], send_sem=ar_s.at[i],
            recv_sem=ag_r.at[i, 2 * o + p], device_id=z_peer(k), device_id_type=MESH)

    def copies_relay(i, side, o, p):
        return pltpu.make_async_remote_copy(
            src_ref=gath.at[i, side, o, p], dst_ref=gath.at[i, side, o, p],
            send_sem=ar_s.at[i], recv_sem=rl_r.at[i], device_id=partner, device_id_type=MESH)

    def all_of(ref, send_sem, recv_sem):
        return pltpu.make_async_remote_copy(
            src_ref=ref, dst_ref=ref, send_sem=send_sem, recv_sem=recv_sem, device_id=partner, device_id_type=MESH)

    def ar_start(i, lhs, w_ref):
        theirs = pl.ds(pl.multiple_of((1 - core) * DH, DH), DH)
        ours = pl.ds(pl.multiple_of(core * DH, DH), DH)
        part[i, 1 - core] = dot(lhs, w_ref[:, theirs])
        copies_core(i).start()
        part[i, core] = dot(lhs, w_ref[:, ours])

    def ar_chip(i):
        copies_core(i).wait_recv()
        chip_sum[i] = (part[i, core] + core_in[i]).reshape(2, 2, PR, DH)
        for p in range(2):
            copies_rs(i, far, jnp.where(tp < 1 + far, tp, tp - 1), p).start()

            @pl.when(jnp.logical_not(mid))
            def _():
                copies_rs(i, near, jnp.where(tp < 1 + near, tp, tp - 1), p).start()

    def ar_own(i, before):
        @pl.when(mid)
        def _():
            for p in range(2):
                all_of(rs_in.at[i, p], ar_s.at[i], rs_r.at[i, p]).wait_recv()
                total = chip_sum[i, near, p] + rs_in[i, p, 0] + rs_in[i, p, 1] + rs_in[i, p, 2]
                gath[i, core, near, p] = (before(p) + total).astype(BF16).astype(F32)
                for k in (2, 1, 3):
                    copies_ag(i, near, k, p).start()
                copies_relay(i, core, near, p).start()

    def ar_relay(i):
        for p in range(2):
            @pl.when(jnp.logical_not(mid))
            def _():
                copies_ag(i, near, 1, p).wait_recv()
                copies_relay(i, core, near, p).start()

            copies_ag(i, far, 1, p).wait_recv()
            copies_relay(i, core, far, p).start()

    def ar_rows(i):
        all_of(gath.at[i, 1 - core], ar_s.at[i], rl_r.at[i]).wait_recv()
        return jnp.concatenate([gath[i, 0].reshape(N, DH), gath[i, 1].reshape(N, DH)], axis=1)

    def ar_drain(i):
        @pl.when(mid)
        def _():
            all_of(gath.at[pl.ds(0, 2)], ar_s.at[i], rl_r.at[i]).wait_send()

        @pl.when(jnp.logical_not(mid))
        def _():
            all_of(rs_in.at[pl.ds(0, 2)], ar_s.at[i], rl_r.at[i]).wait_send()

    ar_start(0, attn, wob)

    def attend_rest():
        heads = attention(TOK)
        for b in range(1, NB):
            ar_start(b, heads[b * N:(b + 1) * N], wob)

    def own_x(b, p):
        rows = pl.ds(pl.multiple_of(b * N + near * NH + p * PR, 8), PR)
        return jnp.where(core == 0, xb[rows, 0:DH].astype(F32), xb[rows, DH:D].astype(F32))

    def mlp(b):
        rows = ar_rows(b)
        b_t = jnp.transpose(jnp.concatenate([normed(rows, gain(1))] * (TOK // N), axis=0)).astype(BF16)
        act_t[...] = b_t
        if b == 0:
            for copy in loads[5:8]:
                copy.wait()
        for j in range(4):
            gate = dot(wgb[j * 256:(j + 1) * 256], act_t[...])
            up = dot(wub[j * 256:(j + 1) * 256], act_t[...])
            u_t = gate * (1.0 / (1.0 + jnp.exp(-gate))) * up
            u_buf[:, j * 256:(j + 1) * 256] = jnp.transpose(u_t).astype(BF16)
        ar_start(NB + b, u_buf[0:N], wdb)

    def own_resid(b, p):
        return gath[b, core, near, p]

    def final_rows(b):
        rows = ar_rows(NB + b)
        return normed(rows, gain(2))

    lane = lax.broadcasted_iota(jnp.int32, (1, TOK), 1)
    tgt_row = target[...] - shard * VOC

    M_OWN, S_OWN, TGT = 0, 1, 2
    kind = lax.broadcasted_iota(jnp.int32, (8, TOK), 0)
    blank = jnp.where(kind == M_OWN, NEG, 0.0)
    for e in range(NG + 1):
        stat[e] = blank

    def inside(e):
        first_tok, size, _ = GROUPS[e]
        return (lane >= first_tok) & (lane < first_tok + size)

    def turn(vals, e, j, back=False):
        shift = GROUPS[e][0] - j * GROUPS[e][1]
        shift = (-shift if back else shift) % TOK
        return pltpu.roll(vals, shift, 1) if shift else vals

    def packed_targets(e):
        wide = jnp.broadcast_to(tgt_row, (8, TOK))
        packed = turn(wide, e, 0, True)
        for j in range(1, GROUPS[e][2]):
            packed = jnp.where(lane >= j * GROUPS[e][1], turn(wide, e, j, True), packed)
        return packed[0:1]

    def own_update(z, b, rows, hit_row, lo, hi):
        live = (rows >= lo) & (rows < hi)
        zm = jnp.where(live, z, NEG)
        m_old = stat[b, M_OWN:M_OWN + 1]
        m_new = jnp.maximum(m_old, jnp.max(zm, axis=0, keepdims=True))
        s_add = jnp.sum(jnp.exp(zm - m_new), axis=0, keepdims=True)
        stat[b, S_OWN:S_OWN + 1] = stat[b, S_OWN:S_OWN + 1] * jnp.exp(m_old - m_new) + s_add
        stat[b, M_OWN:M_OWN + 1] = m_new
        hit = live & (rows == hit_row)
        stat[b, TGT:TGT + 1] = stat[b, TGT:TGT + 1] + jnp.sum(jnp.where(hit, z, 0.0), axis=0, keepdims=True)

    def packed_rows(e, i):
        rows = C // GROUPS[e][2]
        start = NCH * C * GROUPS[e][0] // TOK + i * rows
        return pl.ds(pl.multiple_of(start, 8), rows)

    def y_copy(e, i):
        where = packed_rows(e, i)
        arrived = y_r.at[e] if e < NG - 1 else y_r.at[e + i]
        return pltpu.make_async_remote_copy(
            src_ref=zsend.at[where], dst_ref=zrecv.at[where], send_sem=y_s.at[0], recv_sem=arrived,
            device_id=across, device_id_type=MESH)

    def next_load(g):
        @pl.when(g + NBUF < (NG + 1) * NCH)
        def _():
            w_load(g + NBUF).start()

    def send(e, start, stop):
        _, size, wide = GROUPS[e]
        rows = C // wide
        hit_row = packed_targets(e) - send_base
        packed_row = lax.broadcasted_iota(jnp.int32, (rows, TOK), 0) + lane // size * rows

        def send_chunk(i, carry):
            g = e * NCH + i
            w_load(g).wait()
            slot = g % NBUF
            acc = dot(wbuf[slot, 0:rows], hid_t[e])
            for j in range(1, wide):
                acc = jnp.where(lane >= j * size, dot(wbuf[slot, j * rows:(j + 1) * rows], hid_t[e]), acc)
            z = acc * INV_TEMP
            zsend[packed_rows(e, i)] = z
            y_copy(e, i).start()
            next_load(g)
            own_update(z, e, packed_row + i * C, hit_row, half * LAP, MID + half * LAP)
            return carry

        lax.fori_loop(start, stop, send_chunk, 0)

    keep_lo = (1 - half) * LAP
    keep_hi = MID + (1 - half) * LAP

    def keep():
        row_id = lax.broadcasted_iota(jnp.int32, (C, TOK), 0)
        hit_row = tgt_row - keep_base
        all_t = hid_t[0]
        for e in range(1, NG):
            all_t = jnp.where(lane >= GROUPS[e][0], hid_t[e], all_t)
        hid_all[...] = all_t

        def keep_chunk(i, carry):
            g = NG * NCH + i
            w_load(g).wait()
            z = dot(wbuf[g % NBUF], hid_all[...]) * INV_TEMP
            zkeep[i] = z
            next_load(g)
            own_update(z, NG, row_id + i * C, hit_row, keep_lo, keep_hi)
            return carry

        lax.fori_loop(0, NCH, keep_chunk, 0)

    def merge():
        for e in range(NG):
            for j in range(GROUPS[e][2]):
                moved = turn(stat[e], e, j)
                m_in, s_in = moved[M_OWN:M_OWN + 1], moved[S_OWN:S_OWN + 1]
                m_old = stat[NG, M_OWN:M_OWN + 1]
                s_old = stat[NG, S_OWN:S_OWN + 1]
                t_old = stat[NG, TGT:TGT + 1]
                m_new = jnp.maximum(m_old, m_in)
                s_new = s_old * jnp.exp(m_old - m_new) + s_in * jnp.exp(m_in - m_new)
                here = inside(e)
                stat[NG, M_OWN:M_OWN + 1] = jnp.where(here, m_new, m_old)
                stat[NG, S_OWN:S_OWN + 1] = jnp.where(here, s_new, s_old)
                stat[NG, TGT:TGT + 1] = jnp.where(here, t_old + moved[TGT:TGT + 1], t_old)

    def pair():
        row_q = lax.broadcasted_iota(jnp.int32, (QR, TOK), 0)

        def section(e, i, q):
            rows = C // GROUPS[e][2]
            start = NCH * C * GROUPS[e][0] // TOK + i * rows + q * QR % rows
            return turn(zrecv[pl.ds(pl.multiple_of(start, 8), QR)], e, q * QR // rows)

        def pair_chunk(i, carry):
            top, total = carry
            y_copy(NG - 1, i).wait_recv()
            for q in range(C // QR):
                rows = row_q + (i * C + q * QR)
                live = (rows >= keep_lo) & (rows < keep_hi)
                own = zkeep[i, q * QR:(q + 1) * QR]
                other = section(0, i, q)
                for e in range(1, NG):
                    other = jnp.where(lane >= GROUPS[e][0], section(e, i, q), other)
                z0 = jnp.where(pol, own, other)
                diff = jnp.where(pol, own - other, other - own)
                zm = jnp.where(live, z0, NEG)
                new_top = jnp.maximum(top, jnp.max(zm, axis=0, keepdims=True))
                total = total * jnp.exp(top - new_top) + jnp.sum(jnp.exp(zm - new_top) * diff, axis=0, keepdims=True)
                top = new_top
            return top, total

        for e in range(NG - 1):
            rows = NCH * C * GROUPS[e][1] // TOK
            all_of(zrecv.at[pl.ds(e * rows, rows)], y_s.at[0], y_r.at[e]).wait_recv()
        return lax.fori_loop(0, NCH, pair_chunk, (jnp.full((1, TOK), NEG, F32), jnp.zeros((1, TOK), F32)))

    def rows_out(b):
        hid_t[b] = jnp.transpose(jnp.concatenate([final_rows(b)] * (TOK // N), axis=0)).astype(BF16)

    steps = [
        ar_chip, lambda b: ar_own(b, functools.partial(own_x, b)), ar_relay, mlp,
        lambda b: ar_chip(NB + b), lambda b: ar_own(NB + b, functools.partial(own_resid, b)), lambda b: ar_relay(NB + b), rows_out,
    ]
    sent = [0] * NG
    for item in ",".join(ORDER).split(","):
        which = "abcd".find(item[0].lower())
        if which < 0:
            attend_rest()
        elif item[0].islower():
            steps[int(item[1:])](which)
        else:
            stop = sent[which] + int(item[1:])
            send(which, sent[which], stop)
            sent[which] = stop
    keep()
    for i in range(2 * NB):
        ar_drain(i)
    merge()

    def share_copy(n, device):
        mine, theirs = ((own_shares, own_in), (cross_shares, cross_in))[n]
        return pltpu.make_async_remote_copy(
            src_ref=mine, dst_ref=theirs.at[me], send_sem=f_s.at[n], recv_sem=f_r.at[n],
            device_id=device, device_id_type=MESH)

    def give(n):
        for step in range(NZ):
            to_z = jnp.where(tp < 2, NZ - 1 - step, step)
            for role in range(4):
                to = to_z * 4 + role

                @pl.when(to != me)
                def _():
                    share_copy(n, (dp, to_z, role)).start()

    def take(n):
        others = (own_in, cross_in)[n].at[pl.ds(0, 15)]
        all_of(others, f_s.at[n], f_r.at[n]).wait_recv()

    def normalizer(model):
        ids = [i for i in range(16) if (i % 4) // 2 == model]
        top = functools.reduce(jnp.maximum, [own_in[i, M_OWN:M_OWN + 1] for i in ids])
        tot = sum(own_in[i, S_OWN:S_OWN + 1] * jnp.exp(own_in[i, M_OWN:M_OWN + 1] - top) for i in ids)
        return top, tot

    own_shares[...] = stat[NG, 0:4]
    give(0)
    own_in[me] = stat[NG, 0:4]
    mine = jnp.concatenate(pair(), axis=0)
    cross_shares[...] = mine
    give(1)
    cross_in[me] = mine
    take(0)
    top0, tot0 = normalizer(0)
    top1, tot1 = normalizer(1)
    lse0, lse1 = top0 + jnp.log(tot0), top1 + jnp.log(tot1)
    tgt_z = sum(own_in[i, TGT:TGT + 1] for i in range(16) if (i % 4) // 2 == 0)
    take(1)
    cross = sum(cross_in[i, 1:2] * jnp.exp(cross_in[i, 0:1] - top0) for i in range(16))
    out[...] = jnp.concatenate([cross / tot0 - lse0 + lse1, tgt_z - lse0], axis=0)

    all_of(zsend, y_s.at[0], f_r.at[0]).wait_send()
    all_of(own_in.at[pl.ds(0, 15)], f_s.at[0], f_r.at[0]).wait_send()
    all_of(cross_in.at[pl.ds(0, 15)], f_s.at[1], f_r.at[1]).wait_send()


def solution(mesh):
    by_shard = P(("role", "tp"), None)
    by_role = P("role", None)

    def per_device(hidden, segment_ids, loss_mask, target, norm_gains, w_query, b_query, w_key, b_key, w_value, b_value, w_out, w_gate, w_up, w_down, w_head):
        anywhere = pl.BlockSpec(memory_space=pl.ANY)
        vmem = pl.BlockSpec(memory_space=pltpu.VMEM)
        dma = pltpu.SemaphoreType.DMA
        pair = pl.pallas_call(
            kernel,
            out_shape=jax.ShapeDtypeStruct((2, TOK), F32),
            in_specs=[anywhere] * 10 + [vmem] * 5,
            out_specs=vmem,
            scratch_shapes=[
                pltpu.VMEM((TOK, D), BF16),
                pltpu.VMEM((3, 2, D), F32),
                pltpu.VMEM((384, D), BF16),
                pltpu.VMEM((256, D), BF16),
                pltpu.VMEM((FF, D), BF16),
                pltpu.VMEM((FF, D), BF16),
                pltpu.VMEM((FF, D), BF16),
                pltpu.VMEM((NBUF, C, D), BF16),
                pltpu.VMEM((TOK, TOK), F32),
                pltpu.VMEM((D, TOK), BF16),
                pltpu.VMEM((2 * NB, 2, N, DH), F32),
                pltpu.VMEM((2 * NB, N, DH), F32),
                pltpu.VMEM((2 * NB, 2, 2, PR, DH), F32),
                pltpu.VMEM((2 * NB, 2, 3, PR, DH), F32),
                pltpu.VMEM((2 * NB, 2, 2, 2, PR, DH), F32),
                pltpu.VMEM((NG, D, TOK), BF16),
                pltpu.VMEM((D, TOK), BF16),
                pltpu.VMEM((TOK, FF), BF16),
                pltpu.VMEM((BLK, TOK), F32),
                pltpu.VMEM((BLK, TOK), F32),
                pltpu.VMEM((NCH, C, TOK), F32),
                pltpu.VMEM((NG + 1, 8, TOK), F32),
                pltpu.VMEM((4, TOK), F32),
                pltpu.VMEM((16, 4, TOK), F32),
                pltpu.VMEM((2, TOK), F32),
                pltpu.VMEM((16, 2, TOK), F32),
                dma((9,)), dma((NBUF,)),
                dma((2 * NB,)), dma((2 * NB,)), dma((2 * NB, 2)), dma((2 * NB, 4)), dma((2 * NB,)),
                dma((1,)), dma((NG - 1 + NCH,)), dma((2,)), dma((2,)),
            ],
            compiler_params=pltpu.CompilerParams(
                collective_id=0, has_side_effects=True, vmem_limit_bytes=60 * 1024 * 1024),
        )(hidden, w_query, w_key, w_value, w_out, w_gate, w_up, w_down, w_head, jnp.swapaxes(norm_gains, 0, 1),
          segment_ids.reshape(1, TOK), target.reshape(1, TOK), b_query, b_key, b_value)
        found = loss_mask.astype(F32)
        return pair[0] * found, pair[1] * found

    in_specs = (P(None, "dp", None), P("dp"), P("dp"), P("dp"), P(None, None, None), by_shard, by_shard, by_role, by_role, by_role, by_role, by_shard, by_shard, by_shard, by_shard, by_shard)
    return jax.shard_map(per_device, mesh=mesh, in_specs=in_specs, out_specs=(P("dp"), P("dp")), check_vma=False)
```
